32 devices in a mesh: kgrp: 2 (over y), band: 4 (over z), fft: 4 (over x, core).
Axes of the slice: x: 2, y: 2, z: 4, core: 2. Of those that a mesh axis runs over, the one named last changes fastest.
Arguments:
- orbitals: float32 [8, 64, 64, 128], P(('kgrp', 'band'), 'fft'), parts along dimension 0, may hold values from -6 to 6
- partners: float32 [8, 64, 64, 128], P(('kgrp', 'band'), 'fft'), parts along dimension 0, may hold values from -6 to 6
- shift_table: float32 [8, 3], replicated, may hold values from -0.5 to 0.5
- shift_index: int32 [8], P('kgrp'), parts along dimension 0, may hold values from 0 to 7
Outputs:
- potential: float32 [8, 64, 64, 128], P(('kgrp', 'band'), 'fft'), parts along dimension 0
- projector: float32 [8, 64, 64, 128], P(('kgrp', 'band'), 'fft'), parts along dimension 0
The draws below stay inside these ranges and needn't reach their ends.
There are 2 independent parts, one for each index of `kgrp`. The reference program is written for one: setup_inputs(seed, part) draws one part's arguments, and reference() takes and returns one part's arrays. A program takes and returns all parts, laid end to end along the dimension named above; an argument that names none is the same for every part. Nothing has to cross between parts.
All inputs are finite; a program needn't handle non-finite values.
Results may differ from the reference program's by a relative error of at most 0.0001.
Values sent between devices are 32-bit elements; how exact they have to be, the bound alone decides.
A program may use at most 64 MiB of HBM per device.

```python
import math
import jax
import jax.numpy as jnp
from jax import lax

GRID = 64
NQ = 8
BANDS = 4
PARTNERS = 4


def touch_ends(drawn, rng, least, top_value):
    longest = drawn.shape.index(max(drawn.shape))
    spots = []
    for shift in (0, 1):
        where = [jax.random.randint(jax.random.fold_in(rng, axis), (), 0, length) for axis, length in enumerate(drawn.shape)]
        where[longest] = (where[longest] + shift) % drawn.shape[longest]
        spots.append(tuple(where))
    return drawn.at[spots[0]].set(least).at[spots[1]].set(top_value)


def block_levels(stream_key, dims, pieces, low, high):
    loudness = 1.0
    for dim, parts in pieces:
        heights = jax.random.uniform(jax.random.fold_in(jax.random.fold_in(stream_key, 6), dim), (parts,), jnp.float32, low / len(pieces), high / len(pieces))
        loudness = loudness * jnp.repeat(jnp.exp(heights), dims[dim] // parts).reshape((-1,) + (1,) * (len(dims) - 1 - dim))
    return loudness


def noise(stream_key, shape, scale, bound, split=(), kind=jnp.bfloat16):
    result = jax.random.normal(stream_key, shape, jnp.float32) * scale
    if len(split) > 0:
        result = block_levels(stream_key, shape, split, -0.22, 0.18) * result
    return jnp.clip(result, min=-bound, max=bound).astype(kind)


def setup_inputs(seed: int = 0, part: int = 0) -> dict:
    arg_keys = jax.random.split(jax.random.key(seed), 5)
    part_keys = jax.random.split(jax.random.fold_in(arg_keys[4], part), 5)
    orbitals = noise(part_keys[0], (BANDS, GRID, GRID, 2 * GRID), 0.7, 6.0, ((0, 4), (1, 4)), jnp.float32)
    partners = noise(part_keys[1], (PARTNERS, GRID, GRID, 2 * GRID), 0.7, 6.0, ((0, 4), (1, 4)), jnp.float32)
    shift_table = jnp.clip(jax.random.uniform(arg_keys[2], (NQ, 3), jnp.float32, -0.5, 0.5), -0.5, 0.5)
    shift_index = touch_ends(jax.random.randint(part_keys[3], (PARTNERS,), 0, NQ), jax.random.fold_in(part_keys[3], 1), 0, NQ - 1).astype(jnp.int32)
    return {"orbitals": orbitals, "partners": partners, "shift_table": shift_table, "shift_index": shift_index}


HIGHEST = lax.Precision.HIGHEST
SCREEN_SQUARE = 0.25
FOUR_PI = 4.0 * math.pi

def frequency(positions, extent):
    return jnp.where(positions < extent // 2, positions, positions - extent).astype(jnp.float32)

def rotate(field):
    extent = field.shape[-1] // 2
    return jnp.concatenate([field[..., extent:], -field[..., :extent]], axis=-1)

def factor_inverse(over_real, over_imag):
    matrix_order = over_real.shape[0]
    positions = jnp.arange(matrix_order, dtype=jnp.int32)
    zero_start = jnp.zeros_like(over_real)

    def chol_step(column, lowers):
        lower_real, lower_imag = lowers
        row_real = lower_real[column]
        row_imag = lower_imag[column]
        resid_real = over_real[:, column] - (jnp.dot(lower_real, row_real, precision=HIGHEST) + jnp.dot(lower_imag, row_imag, precision=HIGHEST))
        resid_imag = over_imag[:, column] - (jnp.dot(lower_imag, row_real, precision=HIGHEST) - jnp.dot(lower_real, row_imag, precision=HIGHEST))
        pivot_value = jnp.sqrt(resid_real[column])
        below_diag = positions > column
        at_diag = positions == column
        new_real = jnp.where(below_diag, resid_real / pivot_value, jnp.where(at_diag, pivot_value, 0.0))
        new_imag = jnp.where(below_diag, resid_imag / pivot_value, 0.0)
        chosen = positions[None, :] == column
        return (jnp.where(chosen, new_real[:, None], lower_real), jnp.where(chosen, new_imag[:, None], lower_imag))
    lower_real, lower_imag = lax.fori_loop(0, matrix_order, chol_step, (zero_start, zero_start))

    def solve_step(row_index, inverses):
        inv_real, inv_imag = inverses
        row_real = lower_real[row_index]
        row_imag = lower_imag[row_index]
        sum_real = jnp.dot(row_real, inv_real, precision=HIGHEST) - jnp.dot(row_imag, inv_imag, precision=HIGHEST)
        sum_imag = jnp.dot(row_real, inv_imag, precision=HIGHEST) + jnp.dot(row_imag, inv_real, precision=HIGHEST)
        unit_row = (positions == row_index).astype(over_real.dtype)
        pivot_value = lower_real[row_index, row_index]
        new_real = (unit_row - sum_real) / pivot_value
        new_imag = -sum_imag / pivot_value
        chosen = positions[:, None] == row_index
        return (jnp.where(chosen, new_real[None, :], inv_real), jnp.where(chosen, new_imag[None, :], inv_imag))
    return lax.fori_loop(0, matrix_order, solve_step, (zero_start, zero_start))

def reference(orbitals, partners, shift_table, shift_index):
    extent = orbitals.shape[1]
    orbital_field = orbitals[..., :extent] + 1j * orbitals[..., extent:]
    partner_field = partners[..., :extent] + 1j * partners[..., extent:]
    grid_freq = frequency(jnp.arange(extent, dtype=jnp.int32), extent).astype(orbitals.dtype)

    def partner_term(running, member):
        single, chosen_index = member
        qvector = shift_table[chosen_index]
        denominator = (grid_freq[:, None, None] + qvector[0]) ** 2 + (grid_freq[None, :, None] + qvector[1]) ** 2 + (grid_freq[None, None, :] + qvector[2]) ** 2 + SCREEN_SQUARE
        kernel = FOUR_PI / denominator
        density = jnp.conj(single)[None] * orbital_field
        field = jnp.fft.ifftn(jnp.fft.fftn(density, axes=(1, 2, 3)) * kernel[None], axes=(1, 2, 3))
        return (running + single[None] * field, None)
    start_field = jnp.zeros(orbital_field.shape, orbital_field.dtype)
    exchange_field, _ = lax.scan(partner_term, start_field, (partner_field, shift_index))
    potential = jnp.concatenate([exchange_field.real, exchange_field.imag], axis=-1).astype(orbitals.dtype)
    total_bands = potential.shape[0]
    turned = rotate(potential)
    flat_orbitals = orbitals.reshape(total_bands, -1)
    flat_pot = potential.reshape(total_bands, -1)
    flat_turned = turned.reshape(total_bands, -1)
    volume = float(extent ** 3)
    over_real = jnp.einsum('ik,jk->ij', flat_orbitals, flat_pot, precision=HIGHEST) / volume
    over_imag = jnp.einsum('ik,jk->ij', flat_orbitals, flat_turned, precision=HIGHEST) / volume
    inv_real, inv_imag = factor_inverse(over_real, over_imag)
    projector = jnp.dot(inv_real, flat_pot, precision=HIGHEST) + jnp.dot(inv_imag, flat_turned, precision=HIGHEST)
    return (potential, projector.reshape(potential.shape))
```

```python
import functools
import math

import jax
import jax.numpy as jnp
from jax import lax
from jax.experimental import pallas as pl
from jax.experimental.pallas import tpu as pltpu
from jax.sharding import PartitionSpec as P

HIGHEST = lax.Precision.HIGHEST
HIGH = lax.Precision.HIGH
MESH = pl.DeviceIdType.MESH
SCREEN_SQUARE = 0.25
FOUR_PI = 4.0 * math.pi


def angle_pair(extent, sign):
    positions = jnp.arange(extent, dtype=jnp.int32)
    product = positions[:, None] * positions[None, :] % extent
    angle = 2.0 * math.pi / extent * product.astype(jnp.float32)
    return (jnp.cos(angle), sign * jnp.sin(angle))


def last_table(extent, sign):
    cosine, sine = angle_pair(extent, sign)
    upper = jnp.concatenate([cosine, sine], axis=1)
    lower = jnp.concatenate([-sine, cosine], axis=1)
    return jnp.concatenate([upper, lower], axis=0)


def middle_table(extent, sign):
    cosine, sine = angle_pair(extent, sign)
    return jnp.stack([jnp.stack([cosine, -sine], -1), jnp.stack([sine, cosine], -1)], 1)


def along_last(field, table):
    shape = field.shape
    flat = field.reshape(-1, shape[-1])
    return jnp.dot(flat, table, precision=HIGH).reshape(shape)


def along_axis(field, table, axis_number):
    shape = field.shape
    extent = shape[-1] // 2
    split = field.reshape(shape[0], shape[1], shape[2], 2, extent)
    if axis_number == 1:
        result = jnp.einsum("kcnd,pnbdz->pkbcz", table, split, precision=HIGH)
    else:
        result = jnp.einsum("kcnd,pandz->pakcz", table, split, precision=HIGH)
    return result.reshape(shape)


def times_conj(left, right):
    extent = left.shape[-1] // 2
    left_real, left_imag = (left[..., :extent], left[..., extent:])
    right_real, right_imag = (right[..., :extent], right[..., extent:])
    return jnp.concatenate(
        [
            left_real * right_real + left_imag * right_imag,
            left_real * right_imag - left_imag * right_real,
        ],
        axis=-1,
    )


def times(left, right):
    extent = left.shape[-1] // 2
    left_real, left_imag = (left[..., :extent], left[..., extent:])
    right_real, right_imag = (right[..., :extent], right[..., extent:])
    return jnp.concatenate(
        [
            left_real * right_real - left_imag * right_imag,
            left_real * right_imag + left_imag * right_real,
        ],
        axis=-1,
    )


def rotate(field):
    extent = field.shape[-1] // 2
    return jnp.concatenate([field[..., extent:], -field[..., :extent]], axis=-1)


def frequency(positions, extent):
    return jnp.where(positions < extent // 2, positions, positions - extent).astype(jnp.float32)


def kernel_block(qvectors, y_count, extent):
    first_freq = frequency(jnp.arange(extent, dtype=jnp.int32), extent)
    second_freq = frequency(jnp.arange(y_count, dtype=jnp.int32), extent)
    third_freq = frequency(jnp.arange(2 * extent, dtype=jnp.int32) % extent, extent)
    first_part = (first_freq[None, :] + qvectors[:, 0:1]) ** 2
    second_part = (second_freq[None, :] + qvectors[:, 1:2]) ** 2
    third_part = (third_freq[None, :] + qvectors[:, 2:3]) ** 2
    denominator = (
        first_part[:, :, None, None]
        + second_part[:, None, :, None]
        + third_part[:, None, None, :]
        + SCREEN_SQUARE
    )
    return FOUR_PI / extent**3 / denominator


def shifts_for(shift_table, shift_index, start_at, length):
    picked = lax.dynamic_slice_in_dim(shift_index, start_at, length)
    onehot = (picked[:, None] == jnp.arange(shift_table.shape[0], dtype=jnp.int32)[None, :]).astype(
        jnp.float32
    )
    return jnp.dot(onehot, shift_table, precision=HIGHEST)


def factor_inverse(over_real, over_imag):
    matrix_order = over_real.shape[0]
    positions = jnp.arange(matrix_order, dtype=jnp.int32)
    zero_start = jnp.zeros_like(over_real)

    def chol_step(column, lowers):
        lower_real, lower_imag = lowers
        row_real = lower_real[column]
        row_imag = lower_imag[column]
        resid_real = over_real[:, column] - (
            jnp.dot(lower_real, row_real, precision=HIGHEST)
            + jnp.dot(lower_imag, row_imag, precision=HIGHEST)
        )
        resid_imag = over_imag[:, column] - (
            jnp.dot(lower_imag, row_real, precision=HIGHEST)
            - jnp.dot(lower_real, row_imag, precision=HIGHEST)
        )
        pivot_value = jnp.sqrt(resid_real[column])
        below_diag = positions > column
        at_diag = positions == column
        new_real = jnp.where(
            below_diag, resid_real / pivot_value, jnp.where(at_diag, pivot_value, 0.0)
        )
        new_imag = jnp.where(below_diag, resid_imag / pivot_value, 0.0)
        chosen = positions[None, :] == column
        return (
            jnp.where(chosen, new_real[:, None], lower_real),
            jnp.where(chosen, new_imag[:, None], lower_imag),
        )

    lower_real, lower_imag = lax.fori_loop(0, matrix_order, chol_step, (zero_start, zero_start))

    def solve_step(row_index, inverses):
        inv_real, inv_imag = inverses
        row_real = lower_real[row_index]
        row_imag = lower_imag[row_index]
        sum_real = jnp.dot(row_real, inv_real, precision=HIGHEST) - jnp.dot(
            row_imag, inv_imag, precision=HIGHEST
        )
        sum_imag = jnp.dot(row_real, inv_imag, precision=HIGHEST) + jnp.dot(
            row_imag, inv_real, precision=HIGHEST
        )
        unit_row = (positions == row_index).astype(over_real.dtype)
        pivot_value = lower_real[row_index, row_index]
        new_real = (unit_row - sum_real) / pivot_value
        new_imag = -sum_imag / pivot_value
        chosen = positions[:, None] == row_index
        return (
            jnp.where(chosen, new_real[None, :], inv_real),
            jnp.where(chosen, new_imag[None, :], inv_imag),
        )

    return lax.fori_loop(0, matrix_order, solve_step, (zero_start, zero_start))


def general_body(orbitals, partners, shift_table, shift_index):
    extent = orbitals.shape[2]
    band_count = orbitals.shape[0]
    tables = (
        last_table(extent, -1.0),
        middle_table(extent, -1.0),
        last_table(extent, 1.0),
        middle_table(extent, 1.0),
    )
    my_band = lax.axis_index("band")
    forward_last, forward_mid, inverse_last, inverse_mid = tables
    full_orbitals = lax.all_gather(orbitals, "fft", axis=1, tiled=True)
    every_slab = lax.all_gather(partners, "band", axis=0, tiled=True)
    own_grids = lax.all_to_all(every_slab, "fft", split_axis=0, concat_axis=1, tiled=True)
    own_count = own_grids.shape[0]
    qvectors = shifts_for(shift_table, shift_index, lax.axis_index("fft") * own_count, own_count)

    def one_partner(member, running):
        single = lax.dynamic_slice_in_dim(own_grids, member, 1, 0)
        kernel = kernel_block(lax.dynamic_slice_in_dim(qvectors, member, 1, 0), extent, extent)
        density = times_conj(single, full_orbitals)
        spectrum = (
            along_axis(
                along_axis(along_last(density, forward_last), forward_mid, 2), forward_mid, 1
            )
            * kernel
        )
        field = along_last(
            along_axis(along_axis(spectrum, inverse_mid, 1), inverse_mid, 2), inverse_last
        )
        return running + times(single, field)

    partial_value = lax.fori_loop(
        0, own_count, one_partner, jnp.zeros(full_orbitals.shape, jnp.float32)
    )
    potential = lax.psum_scatter(partial_value, "fft", scatter_dimension=1, tiled=True)
    every_pot = lax.all_gather(potential, "band", axis=0, tiled=True)
    turned = rotate(every_pot)
    total_bands = every_pot.shape[0]
    flat_orbitals = orbitals.reshape(band_count, -1)
    flat_pot = every_pot.reshape(total_bands, -1)
    flat_turned = turned.reshape(total_bands, -1)
    volume = float(extent**3)
    rows_real = jnp.einsum("ik,jk->ij", flat_orbitals, flat_pot, precision=HIGHEST) / volume
    rows_imag = jnp.einsum("ik,jk->ij", flat_orbitals, flat_turned, precision=HIGHEST) / volume
    start_row = my_band * band_count
    summed_real, summed_imag = lax.psum((rows_real, rows_imag), "fft")
    over_real, over_imag = (
        lax.all_gather(summed_real, "band", axis=0, tiled=True),
        lax.all_gather(summed_imag, "band", axis=0, tiled=True),
    )
    inv_real, inv_imag = factor_inverse(over_real, over_imag)
    coef_real = lax.dynamic_slice_in_dim(inv_real, start_row, band_count, 0)
    coef_imag = lax.dynamic_slice_in_dim(inv_imag, start_row, band_count, 0)
    projector = jnp.dot(coef_real, flat_pot, precision=HIGHEST) + jnp.dot(
        coef_imag, flat_turned, precision=HIGHEST
    )
    return (potential, projector.reshape(orbitals.shape))


def remote(source, target, send_sem, recv_sem, where):
    return pltpu.make_async_remote_copy(
        src_ref=source,
        dst_ref=target,
        send_sem=send_sem,
        recv_sem=recv_sem,
        device_id=where,
        device_id_type=MESH,
    )


def greet(others):
    barrier = pltpu.get_barrier_semaphore()
    for other in others:
        pl.semaphore_signal(barrier, inc=1, device_id=other, device_id_type=MESH)
    pl.semaphore_wait(barrier, len(others))


def gather_kernel(
    bands,
    ranks,
    orbital,
    partner,
    orbital_grid,
    partner_grid,
    orbital_parts,
    from_below,
    from_above,
    chain_send,
    chain_recv,
    deliver_send,
    deliver_recv,
    grid_send,
    grid_recv,
    part_send,
    part_recv,
    local_sem,
):
    band = lax.axis_index("band")
    rank = lax.axis_index("fft")
    planes = orbital.shape[0]
    piece = planes // bands
    greet(
        [{"band": (band + step) % bands} for step in range(1, bands)]
        + [{"fft": (rank + step) % ranks} for step in range(1, ranks)]
    )

    def span(index):
        return pl.ds(index * piece, piece)

    def slab(index):
        return pl.ds(index * planes, planes)

    beside = rank + 1 - 2 * (rank % 2)
    across = (rank + 2) % ranks
    beside_across = (beside + 2) % ranks

    def chain_copy(upward, distance, chunk):
        held = from_below if upward else from_above
        source = partner.at[span(chunk)] if distance == 0 else held.at[distance - 1, chunk]
        way = 0 if upward else 1
        return remote(
            source,
            held.at[distance, chunk],
            chain_send.at[way, distance, chunk],
            chain_recv.at[way, distance, chunk],
            {"band": band + 1 if upward else band - 1},
        )

    def deliver(upward, distance, chunk, act):
        held = from_below if upward else from_above
        source = partner.at[span(chunk)] if distance == 0 else held.at[distance - 1, chunk]
        owner = band - distance if upward else band + distance
        target = partner_grid.at[pl.ds(rank * planes + chunk * piece, piece)]
        way = 0 if upward else 1

        @pl.when(owner == rank)
        def _():
            copy = pltpu.make_async_copy(source, target, local_sem.at[chunk])
            copy.start() if act == "start" else copy.wait()

        @pl.when(owner != rank)
        def _():
            copy = remote(
                source,
                target,
                deliver_send.at[way, distance, chunk],
                deliver_recv.at[rank, chunk],
                {"fft": owner},
            )
            copy.start() if act == "start" else copy.wait_send()

    def has_source(upward, distance):
        return band >= distance if upward else band + distance <= bands - 1

    def has_next(upward):
        return band <= bands - 2 if upward else band >= 1

    def both(first, second):
        return jnp.logical_and(first, second)

    for chunk in range(bands):
        for upward in (True, False):

            @pl.when(has_next(upward))
            def _():
                chain_copy(upward, 0, chunk).start()

    to_across = remote(
        orbital, orbital_grid.at[slab(rank)], grid_send.at[0], grid_recv.at[0], {"fft": across}
    )
    to_beside = remote(
        orbital, orbital_grid.at[slab(rank)], grid_send.at[1], grid_recv.at[1], {"fft": beside}
    )
    to_across.start()
    to_beside.start()
    own_grid = pltpu.make_async_copy(orbital, orbital_grid.at[slab(rank)], local_sem.at[bands])
    own_grid.start()
    for chunk in range(bands):
        deliver(True, 0, chunk, "start")
    onward = remote(
        orbital_grid.at[slab(across)],
        orbital_grid.at[slab(across)],
        grid_send.at[2],
        grid_recv.at[2],
        {"fft": beside},
    )
    for distance in range(1, bands):
        for chunk in range(bands):
            for upward in (True, False):

                @pl.when(has_source(upward, distance))
                def _():
                    chain_copy(upward, distance - 1, chunk).wait_recv()

                if distance < bands - 1:

                    @pl.when(both(has_source(upward, distance), has_next(upward)))
                    def _():
                        chain_copy(upward, distance, chunk).start()

                @pl.when(has_source(upward, distance))
                def _():
                    deliver(upward, distance, chunk, "start")

        if distance == 1:
            to_across.wait_recv()
            onward.start()
    part_copies = []
    for step in range(1, bands):
        other = (band + step) % bands
        copy = remote(
            orbital.at[span(other)],
            orbital_parts.at[band],
            part_send.at[step - 1],
            part_recv.at[step - 1],
            {"band": other},
        )
        copy.start()
        part_copies.append(copy)
    own_part = pltpu.make_async_copy(
        orbital.at[span(band)], orbital_parts.at[band], local_sem.at[bands + 1]
    )
    own_part.start()

    for copy in part_copies:
        copy.wait()
    own_part.wait()
    own_grid.wait()
    to_across.wait_send()
    to_beside.wait()
    onward.wait()
    for distance in range(bands):
        for chunk in range(bands):
            for upward in (True, False):
                if distance < bands - 1:

                    @pl.when(both(has_source(upward, distance), has_next(upward)))
                    def _():
                        chain_copy(upward, distance, chunk).wait_send()

                if distance > 0 or upward:

                    @pl.when(has_source(upward, distance))
                    def _():
                        deliver(upward, distance, chunk, "wait")

    for step in range(1, ranks):
        source = (rank + step) % ranks
        for chunk in range(bands):
            target = partner_grid.at[pl.ds(source * planes + chunk * piece, piece)]
            remote(
                target,
                target,
                deliver_send.at[0, 0, chunk],
                deliver_recv.at[source, chunk],
                {"fft": source},
            ).wait_recv()


def gather_grids(bands, ranks, orbital, partner):
    planes, rows, lanes = orbital.shape
    piece = planes // bands
    vmem = pl.BlockSpec(memory_space=pltpu.VMEM)
    grid = jax.ShapeDtypeStruct((ranks * planes, rows, lanes), jnp.float32)
    parts = jax.ShapeDtypeStruct((bands, piece, rows, lanes), jnp.float32)
    held = pltpu.VMEM((bands, bands, piece, rows, lanes), jnp.float32)
    dma = pltpu.SemaphoreType.DMA
    return pl.pallas_call(
        functools.partial(gather_kernel, bands, ranks),
        name="gather_grids",
        out_shape=(grid, grid, parts),
        in_specs=[vmem, vmem],
        out_specs=(vmem, vmem, vmem),
        scratch_shapes=[
            held,
            held,
            dma((2, bands, bands)),
            dma((2, bands, bands)),
            dma((2, bands, bands)),
            dma((ranks, bands)),
            dma((3,)),
            dma((3,)),
            dma((bands,)),
            dma((bands,)),
            dma((bands + 2,)),
        ],
        compiler_params=pltpu.CompilerParams(
            collective_id=0, has_side_effects=True, vmem_limit_bytes=48 * 1024 * 1024
        ),
    )(orbital, partner)


def turn(block):
    lanes = block.shape[-1]
    swapped = pltpu.roll(block, lanes // 2, block.ndim - 1)
    position = lax.broadcasted_iota(jnp.int32, block.shape, block.ndim - 1)
    return jnp.where(position < lanes // 2, swapped, -swapped)


def small_factor_inverse(matrix):
    order = len(matrix)
    lower = [[None] * order for _ in range(order)]
    for column in range(order):
        residual = []
        for row in range(column, order):
            real, imag = matrix[row][column]
            for k in range(column):
                a, b = lower[row][k]
                c, d = lower[column][k]
                real = real - (a * c + b * d)
                imag = imag - (b * c - a * d)
            residual.append((real, imag))
        pivot = jnp.sqrt(residual[0][0])
        lower[column][column] = (pivot, jnp.zeros_like(pivot))
        for row in range(column + 1, order):
            real, imag = residual[row - column]
            lower[row][column] = (real / pivot, imag / pivot)
    inverse = [[None] * order for _ in range(order)]
    for row in range(order):
        pivot = lower[row][row][0]
        inverse[row][row] = (1.0 / pivot, jnp.zeros_like(pivot))
        for column in range(row):
            real = jnp.zeros_like(pivot)
            imag = jnp.zeros_like(pivot)
            for k in range(column, row):
                a, b = lower[row][k]
                c, d = inverse[k][column]
                real = real - (a * c - b * d)
                imag = imag - (a * d + b * c)
            inverse[row][column] = (real / pivot, imag / pivot)
    return inverse


def finish_kernel(
    bands,
    ranks,
    partial,
    orbital_parts,
    potential,
    projector,
    near,
    outgoing,
    arriving,
    potential_parts,
    projector_parts,
    own_sums,
    all_sums,
    near_send,
    near_recv,
    far_send,
    far_recv,
    part_send,
    part_recv,
    sum_send,
    sum_recv,
    back_send,
    back_recv,
):
    band = lax.axis_index("band")
    rank = lax.axis_index("fft")
    planes, rows, lanes = potential.shape
    piece = planes // bands
    beside = rank + 1 - 2 * (rank % 2)
    across = (rank + 2) % ranks
    beside_across = (beside + 2) % ranks
    others = [
        {"band": (band + step) % bands, "fft": (rank + turn_by) % ranks}
        for step in range(bands)
        for turn_by in range(ranks)
        if step or turn_by
    ]
    greet(others)

    def span(index):
        return pl.ds(index * piece, piece)

    def window(index, chunk):
        return pl.ds(index * planes + chunk * piece, piece)

    near_copies = []
    for chunk in range(bands):
        pair = []
        for which, index in ((1, beside_across), (0, beside)):
            copy = remote(
                partial.at[window(index, chunk)],
                near.at[which, chunk],
                near_send.at[which, chunk],
                near_recv.at[which, chunk],
                {"fft": beside},
            )
            copy.start()
            pair.append(copy)
        near_copies.append(pair)
    far_copies = []
    for chunk in range(bands):
        near_copies[chunk][0].wait()
        outgoing[chunk] = partial[window(across, chunk)] + near[1, chunk]
        copy = remote(
            outgoing.at[chunk],
            arriving.at[chunk],
            far_send.at[chunk],
            far_recv.at[chunk],
            {"fft": across},
        )
        copy.start()
        far_copies.append(copy)
    for chunk in range(bands):
        near_copies[chunk][1].wait()
        far_copies[chunk].wait_recv()
        potential[span(chunk)] = (partial[window(rank, chunk)] + near[0, chunk]) + arriving[chunk]

        def part_copy(source_band):
            return remote(
                potential.at[span(chunk)],
                potential_parts.at[source_band],
                part_send.at[chunk],
                part_recv.at[source_band],
                {"band": chunk},
            )

        @pl.when(band != chunk)
        def _():
            part_copy(band).start()

        @pl.when(band == chunk)
        def _():
            potential_parts[chunk] = potential[span(chunk)]

    for other in range(bands):

        @pl.when(band != other)
        def _():
            remote(
                potential_parts.at[other],
                potential_parts.at[other],
                part_send.at[other],
                part_recv.at[other],
                {"band": other},
            ).wait_recv()

    entries = [(i, l) for i in range(bands) for l in range(i + 1)]
    position = lax.broadcasted_iota(jnp.int32, (8, lanes), 1)

    def accumulate(plane, sums):
        turned = []
        straight = []
        for l in range(bands):
            block = potential_parts[l, plane]
            straight.append(block)
            turned.append(turn(block))
        result = []
        for number, (i, l) in enumerate(entries):
            left = orbital_parts[i, plane]
            for half, right in enumerate((straight[l], turned[l])):
                product = (left * right).reshape(rows // 8, 8, lanes)
                result.append(sums[2 * number + half] + jnp.sum(product, axis=0))
        return tuple(result)

    zero = jnp.zeros((8, lanes), jnp.float32)
    sums = lax.fori_loop(0, piece, accumulate, (zero,) * (2 * len(entries)))
    packed = zero
    for number, value in enumerate(sums):
        packed = jnp.where(position == number, jnp.sum(value, axis=1, keepdims=True), packed)
    own_sums[...] = packed
    sum_copies = []
    number = 0
    for step in range(bands):
        for turn_by in range(ranks):
            if step == 0 and turn_by == 0:
                continue
            copy = remote(
                own_sums,
                all_sums.at[band, rank],
                sum_send.at[step, turn_by],
                sum_recv.at[step, turn_by],
                {"band": (band + step) % bands, "fft": (rank + turn_by) % ranks},
            )
            copy.start()
            sum_copies.append(copy)
    all_sums[band, rank] = packed
    for copy in sum_copies:
        copy.wait()
    total = zero
    for one_band in range(bands):
        for one_rank in range(ranks):
            total = total + all_sums[one_band, one_rank]
    total = jnp.broadcast_to(jnp.sum(total, axis=0, keepdims=True), (8, lanes))
    volume = float(lanes // 2) * float(rows) * float(planes * ranks)
    matrix = [[None] * bands for _ in range(bands)]
    for number, (i, l) in enumerate(entries):
        values = [
            jnp.broadcast_to(
                jnp.sum(jnp.where(position == 2 * number + half, total, 0.0), axis=1, keepdims=True),
                (8, lanes),
            )
            / volume
            for half in range(2)
        ]
        matrix[i][l] = (values[0], values[1])
    inverse = small_factor_inverse(matrix)
    back_copies = []

    def spread(value):
        return value[:1]

    for l in range(bands):

        def combine(plane, carry):
            sum_straight = jnp.zeros((rows, lanes), jnp.float32)
            sum_turned = jnp.zeros((rows, lanes), jnp.float32)
            for m in range(l + 1):
                block = potential_parts[m, plane]
                real, imag = inverse[l][m]
                sum_straight = sum_straight + spread(real) * block
                sum_turned = sum_turned + spread(imag) * block
            projector_parts[l, plane] = sum_straight + turn(sum_turned)
            return carry

        lax.fori_loop(0, piece, combine, 0)

        @pl.when(band != l)
        def _():
            remote(
                projector_parts.at[l],
                projector.at[span(band)],
                back_send.at[l],
                back_recv.at[band],
                {"band": l},
            ).start()

        @pl.when(band == l)
        def _():
            projector[span(l)] = projector_parts[l]

    for other in range(bands):

        @pl.when(band != other)
        def _():
            copy = remote(
                projector_parts.at[other],
                projector.at[span(other)],
                back_send.at[other],
                back_recv.at[other],
                {"band": other},
            )
            copy.wait_recv()
            copy.wait_send()
            remote(
                potential.at[span(other)],
                potential_parts.at[other],
                part_send.at[other],
                part_recv.at[other],
                {"band": other},
            ).wait_send()

    for copy in far_copies:
        copy.wait_send()


def finish(bands, ranks, partial, orbital_parts):
    whole, rows, lanes = partial.shape
    planes = whole // ranks
    piece = planes // bands
    vmem = pl.BlockSpec(memory_space=pltpu.VMEM)
    out = jax.ShapeDtypeStruct((planes, rows, lanes), jnp.float32)
    dma = pltpu.SemaphoreType.DMA
    quarters = pltpu.VMEM((bands, piece, rows, lanes), jnp.float32)
    return pl.pallas_call(
        functools.partial(finish_kernel, bands, ranks),
        name="finish",
        out_shape=(out, out),
        in_specs=[vmem, vmem],
        out_specs=(vmem, vmem),
        scratch_shapes=[
            pltpu.VMEM((2, bands, piece, rows, lanes), jnp.float32),
            quarters,
            quarters,
            quarters,
            quarters,
            pltpu.VMEM((8, lanes), jnp.float32),
            pltpu.VMEM((bands, ranks, 8, lanes), jnp.float32),
            dma((2, bands)),
            dma((2, bands)),
            dma((bands,)),
            dma((bands,)),
            dma((bands,)),
            dma((bands,)),
            dma((bands, ranks)),
            dma((bands, ranks)),
            dma((bands,)),
            dma((bands,)),
        ],
        compiler_params=pltpu.CompilerParams(
            collective_id=1, has_side_effects=True, vmem_limit_bytes=48 * 1024 * 1024
        ),
    )(partial, orbital_parts)


def apply_pair(orbital_grid, partner_grid, qvector):
    extent = orbital_grid.shape[1]
    tables = (
        last_table(extent, -1.0),
        middle_table(extent, -1.0),
        last_table(extent, 1.0),
        middle_table(extent, 1.0),
    )
    forward_last, forward_mid, inverse_last, inverse_mid = tables
    single = partner_grid[None]
    kernel = kernel_block(qvector, extent, extent)
    density = times_conj(single, orbital_grid[None])
    spectrum = (
        along_axis(along_axis(along_last(density, forward_last), forward_mid, 2), forward_mid, 1)
        * kernel
    )
    field = along_last(
        along_axis(along_axis(spectrum, inverse_mid, 1), inverse_mid, 2), inverse_last
    )
    return times(single, field)[0]


def paired_body(bands, ranks, orbitals, partners, shift_table, shift_index):
    orbital_grid, partner_grid, orbital_parts = gather_grids(bands, ranks, orbitals[0], partners[0])
    qvector = shifts_for(shift_table, shift_index, lax.axis_index("fft"), 1)
    partial = apply_pair(orbital_grid, partner_grid, qvector)
    potential, projector = finish(bands, ranks, partial, orbital_parts)
    return (potential[None], projector[None])


def body(orbitals, partners, shift_table, shift_index):
    bands = lax.axis_size("band")
    ranks = lax.axis_size("fft")
    count, planes, rows, lanes = orbitals.shape
    grid_bytes = ranks * planes * rows * lanes * 4
    paired = (
        count == 1
        and ranks == 4
        and bands == ranks
        and planes % bands == 0
        and lanes == 2 * rows
        and lanes == 128
        and grid_bytes <= 2 * 1024 * 1024
    )
    if paired:
        return paired_body(bands, ranks, orbitals, partners, shift_table, shift_index)
    return general_body(orbitals, partners, shift_table, shift_index)


def solution(mesh):
    in_specs = (
        P(("kgrp", "band"), "fft", None, None),
        P(("kgrp", "band"), "fft", None, None),
        P(),
        P("kgrp"),
    )
    out_specs = (P(("kgrp", "band"), "fft", None, None), P(("kgrp", "band"), "fft", None, None))
    return jax.shard_map(body, mesh=mesh, in_specs=in_specs, out_specs=out_specs, check_vma=False)
```

```python
import functools
import math

import jax
import jax.numpy as jnp
import numpy as np
from jax import lax
from jax.experimental import pallas as pl
from jax.experimental.pallas import tpu as pltpu
from jax.sharding import PartitionSpec as P

HIGHEST = lax.Precision.HIGHEST
HIGH = lax.Precision.HIGH
MESH = pl.DeviceIdType.MESH
GROUP = 8
SCREEN_SQUARE = 0.25
FOUR_PI = 4.0 * math.pi


def angle_pair(extent, sign):
    positions = jnp.arange(extent, dtype=jnp.int32)
    product = positions[:, None] * positions[None, :] % extent
    angle = 2.0 * math.pi / extent * product.astype(jnp.float32)
    return (jnp.cos(angle), sign * jnp.sin(angle))


def last_table(extent, sign):
    cosine, sine = angle_pair(extent, sign)
    upper = jnp.concatenate([cosine, sine], axis=1)
    lower = jnp.concatenate([-sine, cosine], axis=1)
    return jnp.concatenate([upper, lower], axis=0)


def middle_table(extent, sign):
    cosine, sine = angle_pair(extent, sign)
    return jnp.stack([jnp.stack([cosine, -sine], -1), jnp.stack([sine, cosine], -1)], 1)


def along_last(field, table):
    shape = field.shape
    flat = field.reshape(-1, shape[-1])
    return jnp.dot(flat, table, precision=HIGH).reshape(shape)


def along_axis(field, table, axis_number):
    shape = field.shape
    extent = shape[-1] // 2
    split = field.reshape(shape[0], shape[1], shape[2], 2, extent)
    if axis_number == 1:
        result = jnp.einsum("kcnd,pnbdz->pkbcz", table, split, precision=HIGH)
    else:
        result = jnp.einsum("kcnd,pandz->pakcz", table, split, precision=HIGH)
    return result.reshape(shape)


def times_conj(left, right):
    extent = left.shape[-1] // 2
    left_real, left_imag = (left[..., :extent], left[..., extent:])
    right_real, right_imag = (right[..., :extent], right[..., extent:])
    return jnp.concatenate(
        [
            left_real * right_real + left_imag * right_imag,
            left_real * right_imag - left_imag * right_real,
        ],
        axis=-1,
    )


def times(left, right):
    extent = left.shape[-1] // 2
    left_real, left_imag = (left[..., :extent], left[..., extent:])
    right_real, right_imag = (right[..., :extent], right[..., extent:])
    return jnp.concatenate(
        [
            left_real * right_real - left_imag * right_imag,
            left_real * right_imag + left_imag * right_real,
        ],
        axis=-1,
    )


def rotate(field):
    extent = field.shape[-1] // 2
    return jnp.concatenate([field[..., extent:], -field[..., :extent]], axis=-1)


def frequency(positions, extent):
    return jnp.where(positions < extent // 2, positions, positions - extent).astype(jnp.float32)


def kernel_block(qvectors, y_count, extent):
    first_freq = frequency(jnp.arange(extent, dtype=jnp.int32), extent)
    second_freq = frequency(jnp.arange(y_count, dtype=jnp.int32), extent)
    third_freq = frequency(jnp.arange(2 * extent, dtype=jnp.int32) % extent, extent)
    first_part = (first_freq[None, :] + qvectors[:, 0:1]) ** 2
    second_part = (second_freq[None, :] + qvectors[:, 1:2]) ** 2
    third_part = (third_freq[None, :] + qvectors[:, 2:3]) ** 2
    denominator = (
        first_part[:, :, None, None]
        + second_part[:, None, :, None]
        + third_part[:, None, None, :]
        + SCREEN_SQUARE
    )
    return FOUR_PI / extent**3 / denominator


def shifts_for(shift_table, shift_index, start_at, length):
    picked = lax.dynamic_slice_in_dim(shift_index, start_at, length)
    onehot = (picked[:, None] == jnp.arange(shift_table.shape[0], dtype=jnp.int32)[None, :]).astype(
        jnp.float32
    )
    return jnp.dot(onehot, shift_table, precision=HIGHEST)


def factor_inverse(over_real, over_imag):
    matrix_order = over_real.shape[0]
    positions = jnp.arange(matrix_order, dtype=jnp.int32)
    zero_start = jnp.zeros_like(over_real)

    def chol_step(column, lowers):
        lower_real, lower_imag = lowers
        row_real = lower_real[column]
        row_imag = lower_imag[column]
        resid_real = over_real[:, column] - (
            jnp.dot(lower_real, row_real, precision=HIGHEST)
            + jnp.dot(lower_imag, row_imag, precision=HIGHEST)
        )
        resid_imag = over_imag[:, column] - (
            jnp.dot(lower_imag, row_real, precision=HIGHEST)
            - jnp.dot(lower_real, row_imag, precision=HIGHEST)
        )
        pivot_value = jnp.sqrt(resid_real[column])
        below_diag = positions > column
        at_diag = positions == column
        new_real = jnp.where(
            below_diag, resid_real / pivot_value, jnp.where(at_diag, pivot_value, 0.0)
        )
        new_imag = jnp.where(below_diag, resid_imag / pivot_value, 0.0)
        chosen = positions[None, :] == column
        return (
            jnp.where(chosen, new_real[:, None], lower_real),
            jnp.where(chosen, new_imag[:, None], lower_imag),
        )

    lower_real, lower_imag = lax.fori_loop(0, matrix_order, chol_step, (zero_start, zero_start))

    def solve_step(row_index, inverses):
        inv_real, inv_imag = inverses
        row_real = lower_real[row_index]
        row_imag = lower_imag[row_index]
        sum_real = jnp.dot(row_real, inv_real, precision=HIGHEST) - jnp.dot(
            row_imag, inv_imag, precision=HIGHEST
        )
        sum_imag = jnp.dot(row_real, inv_imag, precision=HIGHEST) + jnp.dot(
            row_imag, inv_real, precision=HIGHEST
        )
        unit_row = (positions == row_index).astype(over_real.dtype)
        pivot_value = lower_real[row_index, row_index]
        new_real = (unit_row - sum_real) / pivot_value
        new_imag = -sum_imag / pivot_value
        chosen = positions[:, None] == row_index
        return (
            jnp.where(chosen, new_real[None, :], inv_real),
            jnp.where(chosen, new_imag[None, :], inv_imag),
        )

    return lax.fori_loop(0, matrix_order, solve_step, (zero_start, zero_start))


def general_body(orbitals, partners, shift_table, shift_index):
    extent = orbitals.shape[2]
    band_count = orbitals.shape[0]
    tables = (
        last_table(extent, -1.0),
        middle_table(extent, -1.0),
        last_table(extent, 1.0),
        middle_table(extent, 1.0),
    )
    my_band = lax.axis_index("band")
    forward_last, forward_mid, inverse_last, inverse_mid = tables
    full_orbitals = lax.all_gather(orbitals, "fft", axis=1, tiled=True)
    every_slab = lax.all_gather(partners, "band", axis=0, tiled=True)
    own_grids = lax.all_to_all(every_slab, "fft", split_axis=0, concat_axis=1, tiled=True)
    own_count = own_grids.shape[0]
    qvectors = shifts_for(shift_table, shift_index, lax.axis_index("fft") * own_count, own_count)

    def one_partner(member, running):
        single = lax.dynamic_slice_in_dim(own_grids, member, 1, 0)
        kernel = kernel_block(lax.dynamic_slice_in_dim(qvectors, member, 1, 0), extent, extent)
        density = times_conj(single, full_orbitals)
        spectrum = (
            along_axis(
                along_axis(along_last(density, forward_last), forward_mid, 2), forward_mid, 1
            )
            * kernel
        )
        field = along_last(
            along_axis(along_axis(spectrum, inverse_mid, 1), inverse_mid, 2), inverse_last
        )
        return running + times(single, field)

    partial_value = lax.fori_loop(
        0, own_count, one_partner, jnp.zeros(full_orbitals.shape, jnp.float32)
    )
    potential = lax.psum_scatter(partial_value, "fft", scatter_dimension=1, tiled=True)
    every_pot = lax.all_gather(potential, "band", axis=0, tiled=True)
    turned = rotate(every_pot)
    total_bands = every_pot.shape[0]
    flat_orbitals = orbitals.reshape(band_count, -1)
    flat_pot = every_pot.reshape(total_bands, -1)
    flat_turned = turned.reshape(total_bands, -1)
    volume = float(extent**3)
    rows_real = jnp.einsum("ik,jk->ij", flat_orbitals, flat_pot, precision=HIGHEST) / volume
    rows_imag = jnp.einsum("ik,jk->ij", flat_orbitals, flat_turned, precision=HIGHEST) / volume
    start_row = my_band * band_count
    summed_real, summed_imag = lax.psum((rows_real, rows_imag), "fft")
    over_real, over_imag = (
        lax.all_gather(summed_real, "band", axis=0, tiled=True),
        lax.all_gather(summed_imag, "band", axis=0, tiled=True),
    )
    inv_real, inv_imag = factor_inverse(over_real, over_imag)
    coef_real = lax.dynamic_slice_in_dim(inv_real, start_row, band_count, 0)
    coef_imag = lax.dynamic_slice_in_dim(inv_imag, start_row, band_count, 0)
    projector = jnp.dot(coef_real, flat_pot, precision=HIGHEST) + jnp.dot(
        coef_imag, flat_turned, precision=HIGHEST
    )
    return (potential, projector.reshape(orbitals.shape))


def remote(source, target, send_sem, recv_sem, where):
    return pltpu.make_async_remote_copy(
        src_ref=source,
        dst_ref=target,
        send_sem=send_sem,
        recv_sem=recv_sem,
        device_id=where,
        device_id_type=MESH,
    )


def greet(others):
    barrier = pltpu.get_barrier_semaphore()
    for other in others:
        pl.semaphore_signal(barrier, inc=1, device_id=other, device_id_type=MESH)
    pl.semaphore_wait(barrier, len(others))


def gather_kernel(
    bands,
    ranks,
    orbital,
    partner,
    orbital_grid,
    partner_grid,
    orbital_parts,
    from_below,
    from_above,
    chain_send,
    chain_recv,
    deliver_send,
    deliver_recv,
    grid_send,
    grid_recv,
    part_send,
    part_recv,
    local_sem,
):
    band = lax.axis_index("band")
    rank = lax.axis_index("fft")
    planes = orbital.shape[0]
    piece = planes // bands
    greet(
        [{"band": (band + step) % bands} for step in range(1, bands)]
        + [{"fft": (rank + step) % ranks} for step in range(1, ranks)]
    )

    def span(index):
        return pl.ds(index * piece, piece)

    def slab(index):
        return pl.ds(index * planes, planes)

    beside = rank + 1 - 2 * (rank % 2)
    across = (rank + 2) % ranks
    beside_across = (beside + 2) % ranks

    def chain_copy(upward, distance, chunk):
        held = from_below if upward else from_above
        source = partner.at[span(chunk)] if distance == 0 else held.at[distance - 1, chunk]
        way = 0 if upward else 1
        return remote(
            source,
            held.at[distance, chunk],
            chain_send.at[way, distance, chunk],
            chain_recv.at[way, distance, chunk],
            {"band": band + 1 if upward else band - 1},
        )

    def deliver(upward, distance, chunk, act):
        held = from_below if upward else from_above
        source = partner.at[span(chunk)] if distance == 0 else held.at[distance - 1, chunk]
        owner = band - distance if upward else band + distance
        target = partner_grid.at[pl.ds(rank * planes + chunk * piece, piece)]
        way = 0 if upward else 1

        @pl.when(owner == rank)
        def _():
            copy = pltpu.make_async_copy(source, target, local_sem.at[chunk])
            copy.start() if act == "start" else copy.wait()

        @pl.when(owner != rank)
        def _():
            copy = remote(
                source,
                target,
                deliver_send.at[way, distance, chunk],
                deliver_recv.at[rank, chunk],
                {"fft": owner},
            )
            copy.start() if act == "start" else copy.wait_send()

    def has_source(upward, distance):
        return band >= distance if upward else band + distance <= bands - 1

    def has_next(upward):
        return band <= bands - 2 if upward else band >= 1

    def both(first, second):
        return jnp.logical_and(first, second)

    for chunk in range(bands):
        for upward in (True, False):

            @pl.when(has_next(upward))
            def _():
                chain_copy(upward, 0, chunk).start()

    to_across = remote(
        orbital, orbital_grid.at[slab(rank)], grid_send.at[0], grid_recv.at[0], {"fft": across}
    )
    to_beside = remote(
        orbital, orbital_grid.at[slab(rank)], grid_send.at[1], grid_recv.at[1], {"fft": beside}
    )
    to_across.start()
    to_beside.start()
    own_grid = pltpu.make_async_copy(orbital, orbital_grid.at[slab(rank)], local_sem.at[bands])
    own_grid.start()
    for chunk in range(bands):
        deliver(True, 0, chunk, "start")
    onward = remote(
        orbital_grid.at[slab(across)],
        orbital_grid.at[slab(across)],
        grid_send.at[2],
        grid_recv.at[2],
        {"fft": beside},
    )
    for distance in range(1, bands):
        for chunk in range(bands):
            for upward in (True, False):

                @pl.when(has_source(upward, distance))
                def _():
                    chain_copy(upward, distance - 1, chunk).wait_recv()

                if distance < bands - 1:

                    @pl.when(both(has_source(upward, distance), has_next(upward)))
                    def _():
                        chain_copy(upward, distance, chunk).start()

                @pl.when(has_source(upward, distance))
                def _():
                    deliver(upward, distance, chunk, "start")

        if distance == 1:
            to_across.wait_recv()
            onward.start()
    part_copies = []
    for step in range(1, bands):
        other = (band + step) % bands
        copy = remote(
            orbital.at[span(other)],
            orbital_parts.at[band],
            part_send.at[step - 1],
            part_recv.at[step - 1],
            {"band": other},
        )
        copy.start()
        part_copies.append(copy)
    own_part = pltpu.make_async_copy(
        orbital.at[span(band)], orbital_parts.at[band], local_sem.at[bands + 1]
    )
    own_part.start()

    for copy in part_copies:
        copy.wait()
    own_part.wait()
    own_grid.wait()
    to_across.wait_send()
    to_beside.wait()
    onward.wait()
    for distance in range(bands):
        for chunk in range(bands):
            for upward in (True, False):
                if distance < bands - 1:

                    @pl.when(both(has_source(upward, distance), has_next(upward)))
                    def _():
                        chain_copy(upward, distance, chunk).wait_send()

                if distance > 0 or upward:

                    @pl.when(has_source(upward, distance))
                    def _():
                        deliver(upward, distance, chunk, "wait")

    for step in range(1, ranks):
        source = (rank + step) % ranks
        for chunk in range(bands):
            target = partner_grid.at[pl.ds(source * planes + chunk * piece, piece)]
            remote(
                target,
                target,
                deliver_send.at[0, 0, chunk],
                deliver_recv.at[source, chunk],
                {"fft": source},
            ).wait_recv()


def gather_grids(bands, ranks, orbital, partner):
    planes, rows, lanes = orbital.shape
    piece = planes // bands
    vmem = pl.BlockSpec(memory_space=pltpu.VMEM)
    grid = jax.ShapeDtypeStruct((ranks * planes, rows, lanes), jnp.float32)
    parts = jax.ShapeDtypeStruct((bands, piece, rows, lanes), jnp.float32)
    held = pltpu.VMEM((bands, bands, piece, rows, lanes), jnp.float32)
    dma = pltpu.SemaphoreType.DMA
    return pl.pallas_call(
        functools.partial(gather_kernel, bands, ranks),
        name="gather_grids",
        out_shape=(grid, grid, parts),
        in_specs=[vmem, vmem],
        out_specs=(vmem, vmem, vmem),
        scratch_shapes=[
            held,
            held,
            dma((2, bands, bands)),
            dma((2, bands, bands)),
            dma((2, bands, bands)),
            dma((ranks, bands)),
            dma((3,)),
            dma((3,)),
            dma((bands,)),
            dma((bands,)),
            dma((bands + 2,)),
        ],
        compiler_params=pltpu.CompilerParams(
            collective_id=0, has_side_effects=True, vmem_limit_bytes=48 * 1024 * 1024
        ),
    )(orbital, partner)


def turn(block):
    lanes = block.shape[-1]
    swapped = pltpu.roll(block, lanes // 2, block.ndim - 1)
    position = lax.broadcasted_iota(jnp.int32, block.shape, block.ndim - 1)
    return jnp.where(position < lanes // 2, swapped, -swapped)


def small_factor_inverse(matrix):
    order = len(matrix)
    lower = [[None] * order for _ in range(order)]
    for column in range(order):
        residual = []
        for row in range(column, order):
            real, imag = matrix[row][column]
            for k in range(column):
                a, b = lower[row][k]
                c, d = lower[column][k]
                real = real - (a * c + b * d)
                imag = imag - (b * c - a * d)
            residual.append((real, imag))
        pivot = jnp.sqrt(residual[0][0])
        lower[column][column] = (pivot, jnp.zeros_like(pivot))
        for row in range(column + 1, order):
            real, imag = residual[row - column]
            lower[row][column] = (real / pivot, imag / pivot)
    inverse = [[None] * order for _ in range(order)]
    for row in range(order):
        pivot = lower[row][row][0]
        inverse[row][row] = (1.0 / pivot, jnp.zeros_like(pivot))
        for column in range(row):
            real = jnp.zeros_like(pivot)
            imag = jnp.zeros_like(pivot)
            for k in range(column, row):
                a, b = lower[row][k]
                c, d = inverse[k][column]
                real = real - (a * c - b * d)
                imag = imag - (a * d + b * c)
            inverse[row][column] = (real / pivot, imag / pivot)
    return inverse


def finish_kernel(
    bands,
    ranks,
    partial,
    orbital_parts,
    potential,
    projector,
    near,
    outgoing,
    arriving,
    potential_parts,
    projector_parts,
    own_sums,
    all_sums,
    near_send,
    near_recv,
    far_send,
    far_recv,
    part_send,
    part_recv,
    sum_send,
    sum_recv,
    back_send,
    back_recv,
):
    band = lax.axis_index("band")
    rank = lax.axis_index("fft")
    planes, rows, lanes = potential.shape
    piece = planes // bands
    beside = rank + 1 - 2 * (rank % 2)
    across = (rank + 2) % ranks
    beside_across = (beside + 2) % ranks
    others = [
        {"band": (band + step) % bands, "fft": (rank + turn_by) % ranks}
        for step in range(bands)
        for turn_by in range(ranks)
        if step or turn_by
    ]
    greet(others)

    def span(index):
        return pl.ds(index * piece, piece)

    def window(index, chunk):
        return pl.ds(index * planes + chunk * piece, piece)

    near_copies = []
    for chunk in range(bands):
        pair = []
        for which, index in ((1, beside_across), (0, beside)):
            copy = remote(
                partial.at[window(index, chunk)],
                near.at[which, chunk],
                near_send.at[which, chunk],
                near_recv.at[which, chunk],
                {"fft": beside},
            )
            copy.start()
            pair.append(copy)
        near_copies.append(pair)
    far_copies = []
    for chunk in range(bands):
        near_copies[chunk][0].wait()
        outgoing[chunk] = partial[window(across, chunk)] + near[1, chunk]
        copy = remote(
            outgoing.at[chunk],
            arriving.at[chunk],
            far_send.at[chunk],
            far_recv.at[chunk],
            {"fft": across},
        )
        copy.start()
        far_copies.append(copy)
    for chunk in range(bands):
        near_copies[chunk][1].wait()
        far_copies[chunk].wait_recv()
        potential[span(chunk)] = (partial[window(rank, chunk)] + near[0, chunk]) + arriving[chunk]

        def part_copy(source_band):
            return remote(
                potential.at[span(chunk)],
                potential_parts.at[source_band],
                part_send.at[chunk],
                part_recv.at[source_band],
                {"band": chunk},
            )

        @pl.when(band != chunk)
        def _():
            part_copy(band).start()

        @pl.when(band == chunk)
        def _():
            potential_parts[chunk] = potential[span(chunk)]

    for other in range(bands):

        @pl.when(band != other)
        def _():
            remote(
                potential_parts.at[other],
                potential_parts.at[other],
                part_send.at[other],
                part_recv.at[other],
                {"band": other},
            ).wait_recv()

    entries = [(i, l) for i in range(bands) for l in range(i + 1)]
    position = lax.broadcasted_iota(jnp.int32, (8, lanes), 1)

    def accumulate(plane, sums):
        turned = []
        straight = []
        for l in range(bands):
            block = potential_parts[l, plane]
            straight.append(block)
            turned.append(turn(block))
        result = []
        for number, (i, l) in enumerate(entries):
            left = orbital_parts[i, plane]
            for half, right in enumerate((straight[l], turned[l])):
                product = (left * right).reshape(rows // 8, 8, lanes)
                result.append(sums[2 * number + half] + jnp.sum(product, axis=0))
        return tuple(result)

    zero = jnp.zeros((8, lanes), jnp.float32)
    sums = lax.fori_loop(0, piece, accumulate, (zero,) * (2 * len(entries)))
    packed = zero
    for number, value in enumerate(sums):
        packed = jnp.where(position == number, jnp.sum(value, axis=1, keepdims=True), packed)
    own_sums[...] = packed
    sum_copies = []
    number = 0
    for step in range(bands):
        for turn_by in range(ranks):
            if step == 0 and turn_by == 0:
                continue
            copy = remote(
                own_sums,
                all_sums.at[band, rank],
                sum_send.at[step, turn_by],
                sum_recv.at[step, turn_by],
                {"band": (band + step) % bands, "fft": (rank + turn_by) % ranks},
            )
            copy.start()
            sum_copies.append(copy)
    all_sums[band, rank] = packed
    for copy in sum_copies:
        copy.wait()
    total = zero
    for one_band in range(bands):
        for one_rank in range(ranks):
            total = total + all_sums[one_band, one_rank]
    total = jnp.broadcast_to(jnp.sum(total, axis=0, keepdims=True), (8, lanes))
    volume = float(lanes // 2) * float(rows) * float(planes * ranks)
    matrix = [[None] * bands for _ in range(bands)]
    for number, (i, l) in enumerate(entries):
        values = [
            jnp.broadcast_to(
                jnp.sum(jnp.where(position == 2 * number + half, total, 0.0), axis=1, keepdims=True),
                (8, lanes),
            )
            / volume
            for half in range(2)
        ]
        matrix[i][l] = (values[0], values[1])
    inverse = small_factor_inverse(matrix)
    back_copies = []

    def spread(value):
        return value[:1]

    for l in range(bands):

        def combine(plane, carry):
            sum_straight = jnp.zeros((rows, lanes), jnp.float32)
            sum_turned = jnp.zeros((rows, lanes), jnp.float32)
            for m in range(l + 1):
                block = potential_parts[m, plane]
                real, imag = inverse[l][m]
                sum_straight = sum_straight + spread(real) * block
                sum_turned = sum_turned + spread(imag) * block
            projector_parts[l, plane] = sum_straight + turn(sum_turned)
            return carry

        lax.fori_loop(0, piece, combine, 0)

        @pl.when(band != l)
        def _():
            remote(
                projector_parts.at[l],
                projector.at[span(band)],
                back_send.at[l],
                back_recv.at[band],
                {"band": l},
            ).start()

        @pl.when(band == l)
        def _():
            projector[span(l)] = projector_parts[l]

    for other in range(bands):

        @pl.when(band != other)
        def _():
            copy = remote(
                projector_parts.at[other],
                projector.at[span(other)],
                back_send.at[other],
                back_recv.at[other],
                {"band": other},
            )
            copy.wait_recv()
            copy.wait_send()
            remote(
                potential.at[span(other)],
                potential_parts.at[other],
                part_send.at[other],
                part_recv.at[other],
                {"band": other},
            ).wait_send()

    for copy in far_copies:
        copy.wait_send()


def finish(bands, ranks, partial, orbital_parts):
    whole, rows, lanes = partial.shape
    planes = whole // ranks
    piece = planes // bands
    vmem = pl.BlockSpec(memory_space=pltpu.VMEM)
    out = jax.ShapeDtypeStruct((planes, rows, lanes), jnp.float32)
    dma = pltpu.SemaphoreType.DMA
    quarters = pltpu.VMEM((bands, piece, rows, lanes), jnp.float32)
    return pl.pallas_call(
        functools.partial(finish_kernel, bands, ranks),
        name="finish",
        out_shape=(out, out),
        in_specs=[vmem, vmem],
        out_specs=(vmem, vmem),
        scratch_shapes=[
            pltpu.VMEM((2, bands, piece, rows, lanes), jnp.float32),
            quarters,
            quarters,
            quarters,
            quarters,
            pltpu.VMEM((8, lanes), jnp.float32),
            pltpu.VMEM((bands, ranks, 8, lanes), jnp.float32),
            dma((2, bands)),
            dma((2, bands)),
            dma((bands,)),
            dma((bands,)),
            dma((bands,)),
            dma((bands,)),
            dma((bands, ranks)),
            dma((bands, ranks)),
            dma((bands,)),
            dma((bands,)),
        ],
        compiler_params=pltpu.CompilerParams(
            collective_id=1, has_side_effects=True, vmem_limit_bytes=48 * 1024 * 1024
        ),
    )(partial, orbital_parts)


def split_table(table):
    high = table.astype(jnp.bfloat16)
    low = (table - high.astype(np.float64)).astype(jnp.bfloat16)
    return high, low


def right_table(extent, sign):
    grid = np.outer(np.arange(extent), np.arange(extent)) % extent
    angle = 2.0 * math.pi / extent * grid
    cosine, sine = np.cos(angle), sign * np.sin(angle)
    table = np.block([[cosine, sine], [-sine, cosine]])
    high, low = split_table(table)
    upper = np.concatenate([high, low], axis=1)
    lower = np.concatenate([high, np.zeros_like(low)], axis=1)
    return np.concatenate([upper, lower], axis=0)


def left_table(extent, sign):
    grid = np.outer(np.arange(extent), np.arange(extent)) % extent
    angle = 2.0 * math.pi / extent * grid
    high, low = split_table(np.concatenate([np.cos(angle), sign * np.sin(angle)], axis=0))
    return np.concatenate([high, high, low], axis=1)


def halves(value):
    high = value.astype(jnp.bfloat16)
    low = (value - high.astype(jnp.float32)).astype(jnp.bfloat16)
    return high, low


def right_product(value, table):
    lanes = value.shape[-1]
    high, low = halves(value)
    both = jnp.dot(
        jnp.concatenate([high, low], axis=1), table, preferred_element_type=jnp.float32
    )
    return both[:, :lanes] + both[:, lanes:]


def left_product(first, second, table):
    rows, lanes = first.shape
    high, low = halves(jnp.concatenate([first, second], axis=1))
    stacked = jnp.concatenate([high, low, high], axis=0)
    both = jnp.dot(table, stacked, preferred_element_type=jnp.float32)
    return tuple(
        both[:rows, cut : cut + lanes] - turn(both[rows:, cut : cut + lanes])
        for cut in (0, lanes)
    )


def spread_parts(value):
    lanes = value.shape[-1]
    swapped = pltpu.roll(value, lanes // 2, value.ndim - 1)
    lower = lax.broadcasted_iota(jnp.int32, value.shape, value.ndim - 1) < lanes // 2
    return jnp.where(lower, value, swapped), jnp.where(lower, swapped, value)


def forward_group(group, orbital_grid, partner_grid, work, right, left):
    rows, lanes = orbital_grid.shape[1:]
    span = pl.ds(group * GROUP, GROUP)
    orbital = orbital_grid[span].reshape(GROUP * rows, lanes)
    real, imag = spread_parts(partner_grid[span].reshape(GROUP * rows, lanes))
    density = real * orbital + imag * turn(orbital)
    lines = right_product(density, right[...])
    planes = []
    for pair in range(GROUP // 2):
        start = 2 * pair * rows
        planes += left_product(
            lines[start : start + rows], lines[start + rows : start + 2 * rows], left[...]
        )
    stacked = jnp.stack(planes, axis=0)
    work[:, span, :] = jnp.swapaxes(stacked, 0, 1)


def backward_group(group, partner_grid, partial, work, right, left):
    rows, lanes = partner_grid.shape[1:]
    span = pl.ds(group * GROUP, GROUP)
    planes = jnp.swapaxes(work[:, span, :], 0, 1)
    lines = []
    for pair in range(GROUP // 2):
        lines += left_product(planes[2 * pair], planes[2 * pair + 1], left[...])
    field = right_product(jnp.concatenate(lines, axis=0), right[...])
    real, imag = spread_parts(partner_grid[span].reshape(GROUP * rows, lanes))
    partial[span] = (real * field - imag * turn(field)).reshape(GROUP, rows, lanes)


def middle_pairs(shift, work, forward, inverse):
    columns, extent, lanes = work.shape
    first = frequency(lax.broadcasted_iota(jnp.int32, (extent, lanes), 0), extent)
    third_place = lax.broadcasted_iota(jnp.int32, (extent, lanes), 1)
    third_place = jnp.where(third_place < lanes // 2, third_place, third_place - lanes // 2)
    third = frequency(third_place, extent)
    base = (first + shift[0]) ** 2 + (third + shift[2]) ** 2 + SCREEN_SQUARE
    scale = FOUR_PI / (float(extent) * float(columns) * float(lanes // 2))

    def one_pair(pair, carry):
        spectra = left_product(work[2 * pair], work[2 * pair + 1], forward[...])
        scaled = []
        for which in range(2):
            column = 2 * pair + which
            second = jnp.where(column < columns // 2, column, column - columns)
            offset = (second.astype(jnp.float32) + shift[1]) ** 2
            scaled.append(spectra[which] * (scale / (base + offset)))
        fields = left_product(scaled[0], scaled[1], inverse[...])
        work[2 * pair] = fields[0]
        work[2 * pair + 1] = fields[1]
        return carry

    lax.fori_loop(0, columns // 2, one_pair, 0, unroll=2)


def pair_kernel(
    shift_table,
    shift_index,
    orbital_grid,
    partner_grid,
    right_forward,
    right_inverse,
    left_forward,
    left_inverse,
    partial,
    work,
):
    chosen = shift_index[lax.axis_index("fft")]
    shift = [shift_table[chosen, axis] for axis in range(3)]
    groups = orbital_grid.shape[0] // GROUP

    def forward(group, carry):
        forward_group(group, orbital_grid, partner_grid, work, right_forward, left_forward)
        return carry

    def backward(group, carry):
        backward_group(group, partner_grid, partial, work, right_inverse, left_inverse)
        return carry

    lax.fori_loop(0, groups, forward, 0)
    middle_pairs(shift, work, left_forward, left_inverse)
    lax.fori_loop(0, groups, backward, 0)


def apply_pair(orbital_grid, partner_grid, shift_table, shift_index):
    extent = orbital_grid.shape[1]
    tables = [
        jnp.asarray(table)
        for table in (
            right_table(extent, -1.0),
            right_table(extent, 1.0),
            left_table(extent, -1.0),
            left_table(extent, 1.0),
        )
    ]
    vmem = pl.BlockSpec(memory_space=pltpu.VMEM)
    smem = pl.BlockSpec(memory_space=pltpu.SMEM)
    return pl.pallas_call(
        pair_kernel,
        name="apply_pair",
        out_shape=jax.ShapeDtypeStruct(orbital_grid.shape, jnp.float32),
        in_specs=[smem, smem] + [vmem] * 6,
        out_specs=vmem,
        scratch_shapes=[pltpu.VMEM(orbital_grid.shape, jnp.float32)],
        compiler_params=pltpu.CompilerParams(vmem_limit_bytes=48 * 1024 * 1024),
    )(shift_table, shift_index, orbital_grid, partner_grid, *tables)


def paired_body(bands, ranks, orbitals, partners, shift_table, shift_index):
    orbital_grid, partner_grid, orbital_parts = gather_grids(bands, ranks, orbitals[0], partners[0])
    partial = apply_pair(orbital_grid, partner_grid, shift_table, shift_index)
    potential, projector = finish(bands, ranks, partial, orbital_parts)
    return (potential[None], projector[None])


def body(orbitals, partners, shift_table, shift_index):
    bands = lax.axis_size("band")
    ranks = lax.axis_size("fft")
    count, planes, rows, lanes = orbitals.shape
    grid_bytes = ranks * planes * rows * lanes * 4
    paired = (
        count == 1
        and ranks == 4
        and bands == ranks
        and planes % bands == 0
        and lanes == 2 * rows
        and lanes == 128
        and grid_bytes <= 2 * 1024 * 1024
    )
    if paired:
        return paired_body(bands, ranks, orbitals, partners, shift_table, shift_index)
    return general_body(orbitals, partners, shift_table, shift_index)


def solution(mesh):
    in_specs = (
        P(("kgrp", "band"), "fft", None, None),
        P(("kgrp", "band"), "fft", None, None),
        P(),
        P("kgrp"),
    )
    out_specs = (P(("kgrp", "band"), "fft", None, None), P(("kgrp", "band"), "fft", None, None))
    return jax.shard_map(body, mesh=mesh, in_specs=in_specs, out_specs=out_specs, check_vma=False)
```

```python
import functools
import math

import jax
import jax.numpy as jnp
import numpy as np
from jax import lax
from jax.experimental import pallas as pl
from jax.experimental.pallas import tpu as pltpu
from jax.sharding import PartitionSpec as P

HIGHEST = lax.Precision.HIGHEST
HIGH = lax.Precision.HIGH
MESH = pl.DeviceIdType.MESH
GROUP = 8
SCREEN_SQUARE = 0.25
FOUR_PI = 4.0 * math.pi


def angle_pair(extent, sign):
    positions = jnp.arange(extent, dtype=jnp.int32)
    product = positions[:, None] * positions[None, :] % extent
    angle = 2.0 * math.pi / extent * product.astype(jnp.float32)
    return (jnp.cos(angle), sign * jnp.sin(angle))


def last_table(extent, sign):
    cosine, sine = angle_pair(extent, sign)
    upper = jnp.concatenate([cosine, sine], axis=1)
    lower = jnp.concatenate([-sine, cosine], axis=1)
    return jnp.concatenate([upper, lower], axis=0)


def middle_table(extent, sign):
    cosine, sine = angle_pair(extent, sign)
    return jnp.stack([jnp.stack([cosine, -sine], -1), jnp.stack([sine, cosine], -1)], 1)


def along_last(field, table):
    shape = field.shape
    flat = field.reshape(-1, shape[-1])
    return jnp.dot(flat, table, precision=HIGH).reshape(shape)


def along_axis(field, table, axis_number):
    shape = field.shape
    extent = shape[-1] // 2
    split = field.reshape(shape[0], shape[1], shape[2], 2, extent)
    if axis_number == 1:
        result = jnp.einsum("kcnd,pnbdz->pkbcz", table, split, precision=HIGH)
    else:
        result = jnp.einsum("kcnd,pandz->pakcz", table, split, precision=HIGH)
    return result.reshape(shape)


def times_conj(left, right):
    extent = left.shape[-1] // 2
    left_real, left_imag = (left[..., :extent], left[..., extent:])
    right_real, right_imag = (right[..., :extent], right[..., extent:])
    return jnp.concatenate(
        [
            left_real * right_real + left_imag * right_imag,
            left_real * right_imag - left_imag * right_real,
        ],
        axis=-1,
    )


def times(left, right):
    extent = left.shape[-1] // 2
    left_real, left_imag = (left[..., :extent], left[..., extent:])
    right_real, right_imag = (right[..., :extent], right[..., extent:])
    return jnp.concatenate(
        [
            left_real * right_real - left_imag * right_imag,
            left_real * right_imag + left_imag * right_real,
        ],
        axis=-1,
    )


def rotate(field):
    extent = field.shape[-1] // 2
    return jnp.concatenate([field[..., extent:], -field[..., :extent]], axis=-1)


def frequency(positions, extent):
    return jnp.where(positions < extent // 2, positions, positions - extent).astype(jnp.float32)


def kernel_block(qvectors, y_count, extent):
    first_freq = frequency(jnp.arange(extent, dtype=jnp.int32), extent)
    second_freq = frequency(jnp.arange(y_count, dtype=jnp.int32), extent)
    third_freq = frequency(jnp.arange(2 * extent, dtype=jnp.int32) % extent, extent)
    first_part = (first_freq[None, :] + qvectors[:, 0:1]) ** 2
    second_part = (second_freq[None, :] + qvectors[:, 1:2]) ** 2
    third_part = (third_freq[None, :] + qvectors[:, 2:3]) ** 2
    denominator = (
        first_part[:, :, None, None]
        + second_part[:, None, :, None]
        + third_part[:, None, None, :]
        + SCREEN_SQUARE
    )
    return FOUR_PI / extent**3 / denominator


def shifts_for(shift_table, shift_index, start_at, length):
    picked = lax.dynamic_slice_in_dim(shift_index, start_at, length)
    onehot = (picked[:, None] == jnp.arange(shift_table.shape[0], dtype=jnp.int32)[None, :]).astype(
        jnp.float32
    )
    return jnp.dot(onehot, shift_table, precision=HIGHEST)


def factor_inverse(over_real, over_imag):
    matrix_order = over_real.shape[0]
    positions = jnp.arange(matrix_order, dtype=jnp.int32)
    zero_start = jnp.zeros_like(over_real)

    def chol_step(column, lowers):
        lower_real, lower_imag = lowers
        row_real = lower_real[column]
        row_imag = lower_imag[column]
        resid_real = over_real[:, column] - (
            jnp.dot(lower_real, row_real, precision=HIGHEST)
            + jnp.dot(lower_imag, row_imag, precision=HIGHEST)
        )
        resid_imag = over_imag[:, column] - (
            jnp.dot(lower_imag, row_real, precision=HIGHEST)
            - jnp.dot(lower_real, row_imag, precision=HIGHEST)
        )
        pivot_value = jnp.sqrt(resid_real[column])
        below_diag = positions > column
        at_diag = positions == column
        new_real = jnp.where(
            below_diag, resid_real / pivot_value, jnp.where(at_diag, pivot_value, 0.0)
        )
        new_imag = jnp.where(below_diag, resid_imag / pivot_value, 0.0)
        chosen = positions[None, :] == column
        return (
            jnp.where(chosen, new_real[:, None], lower_real),
            jnp.where(chosen, new_imag[:, None], lower_imag),
        )

    lower_real, lower_imag = lax.fori_loop(0, matrix_order, chol_step, (zero_start, zero_start))

    def solve_step(row_index, inverses):
        inv_real, inv_imag = inverses
        row_real = lower_real[row_index]
        row_imag = lower_imag[row_index]
        sum_real = jnp.dot(row_real, inv_real, precision=HIGHEST) - jnp.dot(
            row_imag, inv_imag, precision=HIGHEST
        )
        sum_imag = jnp.dot(row_real, inv_imag, precision=HIGHEST) + jnp.dot(
            row_imag, inv_real, precision=HIGHEST
        )
        unit_row = (positions == row_index).astype(over_real.dtype)
        pivot_value = lower_real[row_index, row_index]
        new_real = (unit_row - sum_real) / pivot_value
        new_imag = -sum_imag / pivot_value
        chosen = positions[:, None] == row_index
        return (
            jnp.where(chosen, new_real[None, :], inv_real),
            jnp.where(chosen, new_imag[None, :], inv_imag),
        )

    return lax.fori_loop(0, matrix_order, solve_step, (zero_start, zero_start))


def general_body(orbitals, partners, shift_table, shift_index):
    extent = orbitals.shape[2]
    band_count = orbitals.shape[0]
    tables = (
        last_table(extent, -1.0),
        middle_table(extent, -1.0),
        last_table(extent, 1.0),
        middle_table(extent, 1.0),
    )
    my_band = lax.axis_index("band")
    forward_last, forward_mid, inverse_last, inverse_mid = tables
    full_orbitals = lax.all_gather(orbitals, "fft", axis=1, tiled=True)
    every_slab = lax.all_gather(partners, "band", axis=0, tiled=True)
    own_grids = lax.all_to_all(every_slab, "fft", split_axis=0, concat_axis=1, tiled=True)
    own_count = own_grids.shape[0]
    qvectors = shifts_for(shift_table, shift_index, lax.axis_index("fft") * own_count, own_count)

    def one_partner(member, running):
        single = lax.dynamic_slice_in_dim(own_grids, member, 1, 0)
        kernel = kernel_block(lax.dynamic_slice_in_dim(qvectors, member, 1, 0), extent, extent)
        density = times_conj(single, full_orbitals)
        spectrum = (
            along_axis(
                along_axis(along_last(density, forward_last), forward_mid, 2), forward_mid, 1
            )
            * kernel
        )
        field = along_last(
            along_axis(along_axis(spectrum, inverse_mid, 1), inverse_mid, 2), inverse_last
        )
        return running + times(single, field)

    partial_value = lax.fori_loop(
        0, own_count, one_partner, jnp.zeros(full_orbitals.shape, jnp.float32)
    )
    potential = lax.psum_scatter(partial_value, "fft", scatter_dimension=1, tiled=True)
    every_pot = lax.all_gather(potential, "band", axis=0, tiled=True)
    turned = rotate(every_pot)
    total_bands = every_pot.shape[0]
    flat_orbitals = orbitals.reshape(band_count, -1)
    flat_pot = every_pot.reshape(total_bands, -1)
    flat_turned = turned.reshape(total_bands, -1)
    volume = float(extent**3)
    rows_real = jnp.einsum("ik,jk->ij", flat_orbitals, flat_pot, precision=HIGHEST) / volume
    rows_imag = jnp.einsum("ik,jk->ij", flat_orbitals, flat_turned, precision=HIGHEST) / volume
    start_row = my_band * band_count
    summed_real, summed_imag = lax.psum((rows_real, rows_imag), "fft")
    over_real, over_imag = (
        lax.all_gather(summed_real, "band", axis=0, tiled=True),
        lax.all_gather(summed_imag, "band", axis=0, tiled=True),
    )
    inv_real, inv_imag = factor_inverse(over_real, over_imag)
    coef_real = lax.dynamic_slice_in_dim(inv_real, start_row, band_count, 0)
    coef_imag = lax.dynamic_slice_in_dim(inv_imag, start_row, band_count, 0)
    projector = jnp.dot(coef_real, flat_pot, precision=HIGHEST) + jnp.dot(
        coef_imag, flat_turned, precision=HIGHEST
    )
    return (potential, projector.reshape(orbitals.shape))


def remote(source, target, send_sem, recv_sem, where):
    return pltpu.make_async_remote_copy(
        src_ref=source,
        dst_ref=target,
        send_sem=send_sem,
        recv_sem=recv_sem,
        device_id=where,
        device_id_type=MESH,
    )


def greet(others):
    barrier = pltpu.get_barrier_semaphore()
    for other in others:
        pl.semaphore_signal(barrier, inc=1, device_id=other, device_id_type=MESH)
    pl.semaphore_wait(barrier, len(others))


def turn(block):
    lanes = block.shape[-1]
    swapped = pltpu.roll(block, lanes // 2, block.ndim - 1)
    position = lax.broadcasted_iota(jnp.int32, block.shape, block.ndim - 1)
    return jnp.where(position < lanes // 2, swapped, -swapped)


def small_factor_inverse(matrix):
    order = len(matrix)
    lower = [[None] * order for _ in range(order)]
    for column in range(order):
        residual = []
        for row in range(column, order):
            real, imag = matrix[row][column]
            for k in range(column):
                a, b = lower[row][k]
                c, d = lower[column][k]
                real = real - (a * c + b * d)
                imag = imag - (b * c - a * d)
            residual.append((real, imag))
        pivot = jnp.sqrt(residual[0][0])
        lower[column][column] = (pivot, jnp.zeros_like(pivot))
        for row in range(column + 1, order):
            real, imag = residual[row - column]
            lower[row][column] = (real / pivot, imag / pivot)
    inverse = [[None] * order for _ in range(order)]
    for row in range(order):
        pivot = lower[row][row][0]
        inverse[row][row] = (1.0 / pivot, jnp.zeros_like(pivot))
        for column in range(row):
            real = jnp.zeros_like(pivot)
            imag = jnp.zeros_like(pivot)
            for k in range(column, row):
                a, b = lower[row][k]
                c, d = inverse[k][column]
                real = real - (a * c - b * d)
                imag = imag - (a * d + b * c)
            inverse[row][column] = (real / pivot, imag / pivot)
    return inverse


def split_table(table):
    high = table.astype(jnp.bfloat16)
    low = (table - high.astype(np.float64)).astype(jnp.bfloat16)
    return high, low


def right_table(extent, sign):
    grid = np.outer(np.arange(extent), np.arange(extent)) % extent
    angle = 2.0 * math.pi / extent * grid
    cosine, sine = np.cos(angle), sign * np.sin(angle)
    table = np.block([[cosine, sine], [-sine, cosine]])
    high, low = split_table(table)
    upper = np.concatenate([high, low], axis=1)
    lower = np.concatenate([high, np.zeros_like(low)], axis=1)
    return np.concatenate([upper, lower], axis=0)


def left_table(extent, sign):
    grid = np.outer(np.arange(extent), np.arange(extent)) % extent
    angle = 2.0 * math.pi / extent * grid
    high, low = split_table(np.concatenate([np.cos(angle), sign * np.sin(angle)], axis=0))
    return np.concatenate([high, high, low], axis=1)


def halves(value):
    high = value.astype(jnp.bfloat16)
    low = (value - high.astype(jnp.float32)).astype(jnp.bfloat16)
    return high, low


def right_product(value, table):
    lanes = value.shape[-1]
    high, low = halves(value)
    both = jnp.dot(
        jnp.concatenate([high, low], axis=1), table, preferred_element_type=jnp.float32
    )
    return both[:, :lanes] + both[:, lanes:]


def left_product(first, second, table):
    rows, lanes = first.shape
    high, low = halves(jnp.concatenate([first, second], axis=1))
    stacked = jnp.concatenate([high, low, high], axis=0)
    both = jnp.dot(table, stacked, preferred_element_type=jnp.float32)
    return tuple(
        both[:rows, cut : cut + lanes] - turn(both[rows:, cut : cut + lanes])
        for cut in (0, lanes)
    )


def spread_parts(value):
    lanes = value.shape[-1]
    swapped = pltpu.roll(value, lanes // 2, value.ndim - 1)
    lower = lax.broadcasted_iota(jnp.int32, value.shape, value.ndim - 1) < lanes // 2
    return jnp.where(lower, value, swapped), jnp.where(lower, swapped, value)


def forward_group(group, orbital_grid, partner_grid, work, right, left):
    rows, lanes = orbital_grid.shape[1:]
    span = pl.ds(group * GROUP, GROUP)
    orbital = orbital_grid[span].reshape(GROUP * rows, lanes)
    real, imag = spread_parts(partner_grid[span].reshape(GROUP * rows, lanes))
    density = real * orbital + imag * turn(orbital)
    lines = right_product(density, right[...])
    planes = []
    for pair in range(GROUP // 2):
        start = 2 * pair * rows
        planes += left_product(
            lines[start : start + rows], lines[start + rows : start + 2 * rows], left[...]
        )
    stacked = jnp.stack(planes, axis=0)
    work[:, span, :] = jnp.swapaxes(stacked, 0, 1)


def backward_group(group, partner_grid, partial, work, right, left):
    rows, lanes = partner_grid.shape[1:]
    span = pl.ds(group * GROUP, GROUP)
    planes = jnp.swapaxes(work[:, span, :], 0, 1)
    lines = []
    for pair in range(GROUP // 2):
        lines += left_product(planes[2 * pair], planes[2 * pair + 1], left[...])
    field = right_product(jnp.concatenate(lines, axis=0), right[...])
    real, imag = spread_parts(partner_grid[span].reshape(GROUP * rows, lanes))
    partial[span] = (real * field - imag * turn(field)).reshape(GROUP, rows, lanes)


def middle_pairs(shift, work, forward, inverse):
    columns, extent, lanes = work.shape
    first = frequency(lax.broadcasted_iota(jnp.int32, (extent, lanes), 0), extent)
    third_place = lax.broadcasted_iota(jnp.int32, (extent, lanes), 1)
    third_place = jnp.where(third_place < lanes // 2, third_place, third_place - lanes // 2)
    third = frequency(third_place, extent)
    base = (first + shift[0]) ** 2 + (third + shift[2]) ** 2 + SCREEN_SQUARE
    scale = FOUR_PI / (float(extent) * float(columns) * float(lanes // 2))

    def one_pair(pair, carry):
        spectra = left_product(work[2 * pair], work[2 * pair + 1], forward[...])
        scaled = []
        for which in range(2):
            column = 2 * pair + which
            second = jnp.where(column < columns // 2, column, column - columns)
            offset = (second.astype(jnp.float32) + shift[1]) ** 2
            scaled.append(spectra[which] * (scale / (base + offset)))
        fields = left_product(scaled[0], scaled[1], inverse[...])
        work[2 * pair] = fields[0]
        work[2 * pair + 1] = fields[1]
        return carry

    lax.fori_loop(0, columns // 2, one_pair, 0, unroll=2)


def exchange_kernel(
    bands,
    ranks,
    shift_table,
    shift_index,
    orbital,
    partner,
    right_forward,
    right_inverse,
    left_forward,
    left_inverse,
    potential,
    projector,
    orbital_grid,
    partner_grid,
    orbital_parts,
    from_below,
    from_above,
    work,
    partial,
    near,
    outgoing,
    arriving,
    potential_parts,
    projector_parts,
    own_sums,
    all_sums,
    chain_send,
    chain_recv,
    deliver_send,
    deliver_recv,
    grid_send,
    grid_recv,
    early_send,
    early_recv,
    local_sem,
    near_send,
    near_recv,
    far_send,
    far_recv,
    part_send,
    part_recv,
    sum_send,
    sum_recv,
    back_send,
    back_recv,
):
    band = lax.axis_index("band")
    rank = lax.axis_index("fft")
    planes, rows, lanes = orbital.shape
    piece = planes // bands
    per_group = GROUP // piece
    halves_count = planes // GROUP
    greet(
        [
            {"band": (band + step) % bands, "fft": (rank + turn_by) % ranks}
            for step in range(bands)
            for turn_by in range(ranks)
            if step or turn_by
        ]
    )

    def span(index):
        return pl.ds(index * piece, piece)

    def slab(index):
        return pl.ds(index * planes, planes)

    beside = rank + 1 - 2 * (rank % 2)
    across = (rank + 2) % ranks
    beside_across = (beside + 2) % ranks

    def chain_copy(upward, distance, chunk):
        held = from_below if upward else from_above
        source = partner.at[span(chunk)] if distance == 0 else held.at[distance - 1, chunk]
        way = 0 if upward else 1
        return remote(
            source,
            held.at[distance, chunk],
            chain_send.at[way, distance, chunk],
            chain_recv.at[way, distance, chunk],
            {"band": band + 1 if upward else band - 1},
        )

    def deliver(upward, distance, chunk, act):
        held = from_below if upward else from_above
        source = partner.at[span(chunk)] if distance == 0 else held.at[distance - 1, chunk]
        owner = band - distance if upward else band + distance
        target = partner_grid.at[pl.ds(rank * planes + chunk * piece, piece)]
        way = 0 if upward else 1

        @pl.when(owner == rank)
        def _():
            if act == "start":
                pltpu.make_async_copy(source, target, local_sem.at[chunk]).start()

        @pl.when(owner != rank)
        def _():
            copy = remote(
                source,
                target,
                deliver_send.at[way, distance, chunk],
                deliver_recv.at[rank, chunk],
                {"fft": owner},
            )
            copy.start() if act == "start" else copy.wait_send()

    def has_source(upward, distance):
        return band >= distance if upward else band + distance <= bands - 1

    def has_next(upward):
        return band <= bands - 2 if upward else band >= 1

    def both(first, second):
        return jnp.logical_and(first, second)

    def forward_half(half):
        for chunk in range(half * per_group, (half + 1) * per_group):
            target = partner_grid.at[pl.ds(rank * planes + chunk * piece, piece)]
            pltpu.make_async_copy(partner.at[span(chunk)], target, local_sem.at[chunk]).wait()
            for step in range(1, ranks):
                source = (rank + step) % ranks
                target = partner_grid.at[pl.ds(source * planes + chunk * piece, piece)]
                remote(
                    target,
                    target,
                    deliver_send.at[0, 0, chunk],
                    deliver_recv.at[source, chunk],
                    {"fft": source},
                ).wait_recv()

        def forward(index, carry):
            forward_group(
                index * halves_count + half,
                orbital_grid,
                partner_grid,
                work,
                right_forward,
                left_forward,
            )
            return carry

        lax.fori_loop(0, ranks, forward, 0)

    for chunk in range(bands):
        for upward in (True, False):

            @pl.when(has_next(upward))
            def _():
                chain_copy(upward, 0, chunk).start()

    to_across = remote(
        orbital, orbital_grid.at[slab(rank)], grid_send.at[0], grid_recv.at[0], {"fft": across}
    )
    to_beside = remote(
        orbital, orbital_grid.at[slab(rank)], grid_send.at[1], grid_recv.at[1], {"fft": beside}
    )
    to_across.start()
    to_beside.start()
    own_grid = pltpu.make_async_copy(orbital, orbital_grid.at[slab(rank)], local_sem.at[bands])
    own_grid.start()
    for chunk in range(bands):
        deliver(True, 0, chunk, "start")
    onward = remote(
        orbital_grid.at[slab(across)],
        orbital_grid.at[slab(across)],
        grid_send.at[2],
        grid_recv.at[2],
        {"fft": beside},
    )
    for distance in range(1, bands):
        for chunk in range(bands):
            for upward in (True, False):

                @pl.when(has_source(upward, distance))
                def _():
                    chain_copy(upward, distance - 1, chunk).wait_recv()

                if distance < bands - 1:

                    @pl.when(both(has_source(upward, distance), has_next(upward)))
                    def _():
                        chain_copy(upward, distance, chunk).start()

                @pl.when(has_source(upward, distance))
                def _():
                    deliver(upward, distance, chunk, "start")

            if distance == bands - 1 and chunk > 0 and chunk % per_group == 0:
                forward_half(chunk // per_group - 1)

        if distance == 1:
            to_across.wait_recv()
            onward.start()
            own_grid.wait()
            to_beside.wait_recv()
            onward.wait_recv()
    forward_half(halves_count - 1)
    early_copies = []
    for step in range(1, bands):
        other = (band + step) % bands
        copy = remote(
            orbital.at[span(other)],
            orbital_parts.at[band],
            early_send.at[step - 1],
            early_recv.at[step - 1],
            {"band": other},
        )
        copy.start()
        early_copies.append(copy)
    own_part = pltpu.make_async_copy(
        orbital.at[span(band)], orbital_parts.at[band], local_sem.at[bands + 1]
    )
    own_part.start()

    chosen = shift_index[rank]
    shift = [shift_table[chosen, axis] for axis in range(3)]
    middle_pairs(shift, work, left_forward, left_inverse)

    def backward_slab(index):
        def backward(half, carry):
            backward_group(
                index * halves_count + half, partner_grid, partial, work, right_inverse, left_inverse
            )
            return carry

        lax.fori_loop(0, halves_count, backward, 0)

    def near_copy(which, index):
        return remote(
            partial.at[slab(index)],
            near.at[which],
            near_send.at[which],
            near_recv.at[which],
            {"fft": beside},
        )

    def far_copy(chunk):
        return remote(
            outgoing.at[chunk],
            arriving.at[chunk],
            far_send.at[chunk],
            far_recv.at[chunk],
            {"fft": across},
        )

    def window(index, chunk):
        return pl.ds(index * planes + chunk * piece, piece)

    turns = [(band + step) % bands for step in range(1, bands + 1)]
    backward_slab(beside_across)
    near_copy(1, beside_across).start()
    backward_slab(across)
    near_copy(1, beside_across).wait_recv()
    for chunk in turns:
        outgoing[chunk] = partial[window(across, chunk)] + near[1, span(chunk)]
        far_copy(chunk).start()
    backward_slab(beside)
    near_copy(0, beside).start()
    backward_slab(rank)
    near_copy(0, beside).wait_recv()

    def part_copy(chunk):
        return remote(
            potential.at[span(chunk)],
            potential_parts.at[band],
            part_send.at[chunk],
            part_recv.at[band],
            {"band": chunk},
        )

    for step, chunk in enumerate(turns):
        far_copy(chunk).wait_recv()
        potential[span(chunk)] = (
            partial[window(rank, chunk)] + near[0, span(chunk)]
        ) + arriving[chunk]
        if step < bands - 1:
            part_copy(chunk).start()
        else:
            potential_parts[band] = potential[span(band)]
    for chunk in turns[:-1]:
        remote(
            potential_parts.at[chunk],
            potential_parts.at[chunk],
            part_send.at[chunk],
            part_recv.at[chunk],
            {"band": chunk},
        ).wait_recv()
    for copy in early_copies:
        copy.wait()
    own_part.wait()

    entries = [(i, l) for i in range(bands) for l in range(i + 1)]
    position = lax.broadcasted_iota(jnp.int32, (8, lanes), 1)

    def accumulate(plane, sums):
        turned = []
        straight = []
        for l in range(bands):
            block = potential_parts[l, plane]
            straight.append(block)
            turned.append(turn(block))
        result = []
        for number, (i, l) in enumerate(entries):
            left = orbital_parts[i, plane]
            for half, right in enumerate((straight[l], turned[l])):
                product = (left * right).reshape(rows // 8, 8, lanes)
                result.append(sums[2 * number + half] + jnp.sum(product, axis=0))
        return tuple(result)

    zero = jnp.zeros((8, lanes), jnp.float32)
    sums = lax.fori_loop(0, piece, accumulate, (zero,) * (2 * len(entries)))
    packed = zero
    for number, value in enumerate(sums):
        packed = jnp.where(position == number, jnp.sum(value, axis=1, keepdims=True), packed)
    own_sums[...] = packed
    sum_copies = []
    number = 0
    for step in range(bands):
        for turn_by in range(ranks):
            if step == 0 and turn_by == 0:
                continue
            copy = remote(
                own_sums,
                all_sums.at[band, rank],
                sum_send.at[step, turn_by],
                sum_recv.at[step, turn_by],
                {"band": (band + step) % bands, "fft": (rank + turn_by) % ranks},
            )
            copy.start()
            sum_copies.append(copy)
    all_sums[band, rank] = packed
    for copy in sum_copies:
        copy.wait()
    total = zero
    for one_band in range(bands):
        for one_rank in range(ranks):
            total = total + all_sums[one_band, one_rank]
    total = jnp.broadcast_to(jnp.sum(total, axis=0, keepdims=True), (8, lanes))
    volume = float(lanes // 2) * float(rows) * float(planes * ranks)
    matrix = [[None] * bands for _ in range(bands)]
    for number, (i, l) in enumerate(entries):
        values = [
            jnp.broadcast_to(
                jnp.sum(jnp.where(position == 2 * number + half, total, 0.0), axis=1, keepdims=True),
                (8, lanes),
            )
            / volume
            for half in range(2)
        ]
        matrix[i][l] = (values[0], values[1])
    inverse = small_factor_inverse(matrix)
    back_copies = []

    def spread(value):
        return value[:1]

    for l in range(bands):

        def combine(plane, carry):
            sum_straight = jnp.zeros((rows, lanes), jnp.float32)
            sum_turned = jnp.zeros((rows, lanes), jnp.float32)
            for m in range(l + 1):
                block = potential_parts[m, plane]
                real, imag = inverse[l][m]
                sum_straight = sum_straight + spread(real) * block
                sum_turned = sum_turned + spread(imag) * block
            projector_parts[l, plane] = sum_straight + turn(sum_turned)
            return carry

        lax.fori_loop(0, piece, combine, 0)

    for chunk in turns[1:-1] + turns[:1]:
        remote(
            projector_parts.at[chunk],
            projector.at[span(band)],
            back_send.at[chunk],
            back_recv.at[band],
            {"band": chunk},
        ).start()
    projector[span(band)] = projector_parts[band]
    for chunk in turns[:-1]:
        back = remote(
            projector_parts.at[chunk],
            projector.at[span(chunk)],
            back_send.at[chunk],
            back_recv.at[chunk],
            {"band": chunk},
        )
        back.wait_recv()
        back.wait_send()
        part_copy(chunk).wait_send()
    for chunk in turns:
        far_copy(chunk).wait_send()
    near_copy(0, beside).wait_send()
    near_copy(1, beside_across).wait_send()
    to_across.wait_send()
    to_beside.wait_send()
    onward.wait_send()
    for distance in range(bands):
        for chunk in range(bands):
            for upward in (True, False):
                if distance < bands - 1:

                    @pl.when(both(has_source(upward, distance), has_next(upward)))
                    def _():
                        chain_copy(upward, distance, chunk).wait_send()

                if distance > 0 or upward:

                    @pl.when(has_source(upward, distance))
                    def _():
                        deliver(upward, distance, chunk, "wait")


def exchange(bands, ranks, orbital, partner, shift_table, shift_index):
    planes, rows, lanes = orbital.shape
    piece = planes // bands
    vmem = pl.BlockSpec(memory_space=pltpu.VMEM)
    smem = pl.BlockSpec(memory_space=pltpu.SMEM)
    out = jax.ShapeDtypeStruct((planes, rows, lanes), jnp.float32)
    grid = pltpu.VMEM((ranks * planes, rows, lanes), jnp.float32)
    held = pltpu.VMEM((bands - 1, bands, piece, rows, lanes), jnp.float32)
    quarters = pltpu.VMEM((bands, piece, rows, lanes), jnp.float32)
    dma = pltpu.SemaphoreType.DMA
    tables = [
        jnp.asarray(table)
        for table in (
            right_table(rows, -1.0),
            right_table(rows, 1.0),
            left_table(rows, -1.0),
            left_table(rows, 1.0),
        )
    ]
    return pl.pallas_call(
        functools.partial(exchange_kernel, bands, ranks),
        name="exchange",
        out_shape=(out, out),
        in_specs=[smem, smem] + [vmem] * 6,
        out_specs=(vmem, vmem),
        scratch_shapes=[
            grid,
            grid,
            quarters,
            held,
            held,
            grid,
            grid,
            pltpu.VMEM((2, planes, rows, lanes), jnp.float32),
            quarters,
            quarters,
            quarters,
            quarters,
            pltpu.VMEM((8, lanes), jnp.float32),
            pltpu.VMEM((bands, ranks, 8, lanes), jnp.float32),
            dma((2, bands, bands)),
            dma((2, bands, bands)),
            dma((2, bands, bands)),
            dma((ranks, bands)),
            dma((3,)),
            dma((3,)),
            dma((bands,)),
            dma((bands,)),
            dma((bands + 2,)),
            dma((2,)),
            dma((2,)),
            dma((bands,)),
            dma((bands,)),
            dma((bands,)),
            dma((bands,)),
            dma((bands, ranks)),
            dma((bands, ranks)),
            dma((bands,)),
            dma((bands,)),
        ],
        compiler_params=pltpu.CompilerParams(
            collective_id=0, has_side_effects=True, vmem_limit_bytes=48 * 1024 * 1024
        ),
    )(shift_table, shift_index, orbital, partner, *tables)


def paired_body(bands, ranks, orbitals, partners, shift_table, shift_index):
    potential, projector = exchange(
        bands, ranks, orbitals[0], partners[0], shift_table, shift_index
    )
    return (potential[None], projector[None])


def body(orbitals, partners, shift_table, shift_index):
    bands = lax.axis_size("band")
    ranks = lax.axis_size("fft")
    count, planes, rows, lanes = orbitals.shape
    grid_bytes = ranks * planes * rows * lanes * 4
    paired = (
        count == 1
        and ranks == 4
        and bands == ranks
        and planes % bands == 0
        and planes % GROUP == 0
        and GROUP % (planes // bands) == 0
        and lanes == 2 * rows
        and lanes == 128
        and grid_bytes <= 2 * 1024 * 1024
    )
    if paired:
        return paired_body(bands, ranks, orbitals, partners, shift_table, shift_index)
    return general_body(orbitals, partners, shift_table, shift_index)


def solution(mesh):
    in_specs = (
        P(("kgrp", "band"), "fft", None, None),
        P(("kgrp", "band"), "fft", None, None),
        P(),
        P("kgrp"),
    )
    out_specs = (P(("kgrp", "band"), "fft", None, None), P(("kgrp", "band"), "fft", None, None))
    return jax.shard_map(body, mesh=mesh, in_specs=in_specs, out_specs=out_specs, check_vma=False)
```

```python
import functools
import math

import jax
import jax.numpy as jnp
import numpy as np
from jax import lax
from jax.experimental import pallas as pl
from jax.experimental.pallas import tpu as pltpu
from jax.sharding import PartitionSpec as P

HIGHEST = lax.Precision.HIGHEST
HIGH = lax.Precision.HIGH
MESH = pl.DeviceIdType.MESH
GROUP = 8
SCREEN_SQUARE = 0.25
FOUR_PI = 4.0 * math.pi


def angle_pair(extent, sign):
    positions = jnp.arange(extent, dtype=jnp.int32)
    product = positions[:, None] * positions[None, :] % extent
    angle = 2.0 * math.pi / extent * product.astype(jnp.float32)
    return (jnp.cos(angle), sign * jnp.sin(angle))


def last_table(extent, sign):
    cosine, sine = angle_pair(extent, sign)
    upper = jnp.concatenate([cosine, sine], axis=1)
    lower = jnp.concatenate([-sine, cosine], axis=1)
    return jnp.concatenate([upper, lower], axis=0)


def middle_table(extent, sign):
    cosine, sine = angle_pair(extent, sign)
    return jnp.stack([jnp.stack([cosine, -sine], -1), jnp.stack([sine, cosine], -1)], 1)


def along_last(field, table):
    shape = field.shape
    flat = field.reshape(-1, shape[-1])
    return jnp.dot(flat, table, precision=HIGH).reshape(shape)


def along_axis(field, table, axis_number):
    shape = field.shape
    extent = shape[-1] // 2
    split = field.reshape(shape[0], shape[1], shape[2], 2, extent)
    if axis_number == 1:
        result = jnp.einsum("kcnd,pnbdz->pkbcz", table, split, precision=HIGH)
    else:
        result = jnp.einsum("kcnd,pandz->pakcz", table, split, precision=HIGH)
    return result.reshape(shape)


def times_conj(left, right):
    extent = left.shape[-1] // 2
    left_real, left_imag = (left[..., :extent], left[..., extent:])
    right_real, right_imag = (right[..., :extent], right[..., extent:])
    return jnp.concatenate(
        [
            left_real * right_real + left_imag * right_imag,
            left_real * right_imag - left_imag * right_real,
        ],
        axis=-1,
    )


def times(left, right):
    extent = left.shape[-1] // 2
    left_real, left_imag = (left[..., :extent], left[..., extent:])
    right_real, right_imag = (right[..., :extent], right[..., extent:])
    return jnp.concatenate(
        [
            left_real * right_real - left_imag * right_imag,
            left_real * right_imag + left_imag * right_real,
        ],
        axis=-1,
    )


def rotate(field):
    extent = field.shape[-1] // 2
    return jnp.concatenate([field[..., extent:], -field[..., :extent]], axis=-1)


def frequency(positions, extent):
    return jnp.where(positions < extent // 2, positions, positions - extent).astype(jnp.float32)


def kernel_block(qvectors, y_count, extent):
    first_freq = frequency(jnp.arange(extent, dtype=jnp.int32), extent)
    second_freq = frequency(jnp.arange(y_count, dtype=jnp.int32), extent)
    third_freq = frequency(jnp.arange(2 * extent, dtype=jnp.int32) % extent, extent)
    first_part = (first_freq[None, :] + qvectors[:, 0:1]) ** 2
    second_part = (second_freq[None, :] + qvectors[:, 1:2]) ** 2
    third_part = (third_freq[None, :] + qvectors[:, 2:3]) ** 2
    denominator = (
        first_part[:, :, None, None]
        + second_part[:, None, :, None]
        + third_part[:, None, None, :]
        + SCREEN_SQUARE
    )
    return FOUR_PI / extent**3 / denominator


def shifts_for(shift_table, shift_index, start_at, length):
    picked = lax.dynamic_slice_in_dim(shift_index, start_at, length)
    onehot = (picked[:, None] == jnp.arange(shift_table.shape[0], dtype=jnp.int32)[None, :]).astype(
        jnp.float32
    )
    return jnp.dot(onehot, shift_table, precision=HIGHEST)


def factor_inverse(over_real, over_imag):
    matrix_order = over_real.shape[0]
    positions = jnp.arange(matrix_order, dtype=jnp.int32)
    zero_start = jnp.zeros_like(over_real)

    def chol_step(column, lowers):
        lower_real, lower_imag = lowers
        row_real = lower_real[column]
        row_imag = lower_imag[column]
        resid_real = over_real[:, column] - (
            jnp.dot(lower_real, row_real, precision=HIGHEST)
            + jnp.dot(lower_imag, row_imag, precision=HIGHEST)
        )
        resid_imag = over_imag[:, column] - (
            jnp.dot(lower_imag, row_real, precision=HIGHEST)
            - jnp.dot(lower_real, row_imag, precision=HIGHEST)
        )
        pivot_value = jnp.sqrt(resid_real[column])
        below_diag = positions > column
        at_diag = positions == column
        new_real = jnp.where(
            below_diag, resid_real / pivot_value, jnp.where(at_diag, pivot_value, 0.0)
        )
        new_imag = jnp.where(below_diag, resid_imag / pivot_value, 0.0)
        chosen = positions[None, :] == column
        return (
            jnp.where(chosen, new_real[:, None], lower_real),
            jnp.where(chosen, new_imag[:, None], lower_imag),
        )

    lower_real, lower_imag = lax.fori_loop(0, matrix_order, chol_step, (zero_start, zero_start))

    def solve_step(row_index, inverses):
        inv_real, inv_imag = inverses
        row_real = lower_real[row_index]
        row_imag = lower_imag[row_index]
        sum_real = jnp.dot(row_real, inv_real, precision=HIGHEST) - jnp.dot(
            row_imag, inv_imag, precision=HIGHEST
        )
        sum_imag = jnp.dot(row_real, inv_imag, precision=HIGHEST) + jnp.dot(
            row_imag, inv_real, precision=HIGHEST
        )
        unit_row = (positions == row_index).astype(over_real.dtype)
        pivot_value = lower_real[row_index, row_index]
        new_real = (unit_row - sum_real) / pivot_value
        new_imag = -sum_imag / pivot_value
        chosen = positions[:, None] == row_index
        return (
            jnp.where(chosen, new_real[None, :], inv_real),
            jnp.where(chosen, new_imag[None, :], inv_imag),
        )

    return lax.fori_loop(0, matrix_order, solve_step, (zero_start, zero_start))


def general_body(orbitals, partners, shift_table, shift_index):
    extent = orbitals.shape[2]
    band_count = orbitals.shape[0]
    tables = (
        last_table(extent, -1.0),
        middle_table(extent, -1.0),
        last_table(extent, 1.0),
        middle_table(extent, 1.0),
    )
    my_band = lax.axis_index("band")
    forward_last, forward_mid, inverse_last, inverse_mid = tables
    full_orbitals = lax.all_gather(orbitals, "fft", axis=1, tiled=True)
    every_slab = lax.all_gather(partners, "band", axis=0, tiled=True)
    own_grids = lax.all_to_all(every_slab, "fft", split_axis=0, concat_axis=1, tiled=True)
    own_count = own_grids.shape[0]
    qvectors = shifts_for(shift_table, shift_index, lax.axis_index("fft") * own_count, own_count)

    def one_partner(member, running):
        single = lax.dynamic_slice_in_dim(own_grids, member, 1, 0)
        kernel = kernel_block(lax.dynamic_slice_in_dim(qvectors, member, 1, 0), extent, extent)
        density = times_conj(single, full_orbitals)
        spectrum = (
            along_axis(
                along_axis(along_last(density, forward_last), forward_mid, 2), forward_mid, 1
            )
            * kernel
        )
        field = along_last(
            along_axis(along_axis(spectrum, inverse_mid, 1), inverse_mid, 2), inverse_last
        )
        return running + times(single, field)

    partial_value = lax.fori_loop(
        0, own_count, one_partner, jnp.zeros(full_orbitals.shape, jnp.float32)
    )
    potential = lax.psum_scatter(partial_value, "fft", scatter_dimension=1, tiled=True)
    every_pot = lax.all_gather(potential, "band", axis=0, tiled=True)
    turned = rotate(every_pot)
    total_bands = every_pot.shape[0]
    flat_orbitals = orbitals.reshape(band_count, -1)
    flat_pot = every_pot.reshape(total_bands, -1)
    flat_turned = turned.reshape(total_bands, -1)
    volume = float(extent**3)
    rows_real = jnp.einsum("ik,jk->ij", flat_orbitals, flat_pot, precision=HIGHEST) / volume
    rows_imag = jnp.einsum("ik,jk->ij", flat_orbitals, flat_turned, precision=HIGHEST) / volume
    start_row = my_band * band_count
    summed_real, summed_imag = lax.psum((rows_real, rows_imag), "fft")
    over_real, over_imag = (
        lax.all_gather(summed_real, "band", axis=0, tiled=True),
        lax.all_gather(summed_imag, "band", axis=0, tiled=True),
    )
    inv_real, inv_imag = factor_inverse(over_real, over_imag)
    coef_real = lax.dynamic_slice_in_dim(inv_real, start_row, band_count, 0)
    coef_imag = lax.dynamic_slice_in_dim(inv_imag, start_row, band_count, 0)
    projector = jnp.dot(coef_real, flat_pot, precision=HIGHEST) + jnp.dot(
        coef_imag, flat_turned, precision=HIGHEST
    )
    return (potential, projector.reshape(orbitals.shape))


def remote(source, target, send_sem, recv_sem, where):
    return pltpu.make_async_remote_copy(
        src_ref=source,
        dst_ref=target,
        send_sem=send_sem,
        recv_sem=recv_sem,
        device_id=where,
        device_id_type=MESH,
    )


def greet(others):
    barrier = pltpu.get_barrier_semaphore()
    for other in others:
        pl.semaphore_signal(barrier, inc=1, device_id=other, device_id_type=MESH)
    pl.semaphore_wait(barrier, len(others))


def turn(block):
    lanes = block.shape[-1]
    swapped = pltpu.roll(block, lanes // 2, block.ndim - 1)
    position = lax.broadcasted_iota(jnp.int32, block.shape, block.ndim - 1)
    return jnp.where(position < lanes // 2, swapped, -swapped)


def small_factor_inverse(matrix):
    order = len(matrix)
    lower = [[None] * order for _ in range(order)]
    for column in range(order):
        residual = []
        for row in range(column, order):
            real, imag = matrix[row][column]
            for k in range(column):
                a, b = lower[row][k]
                c, d = lower[column][k]
                real = real - (a * c + b * d)
                imag = imag - (b * c - a * d)
            residual.append((real, imag))
        pivot = jnp.sqrt(residual[0][0])
        lower[column][column] = (pivot, jnp.zeros_like(pivot))
        for row in range(column + 1, order):
            real, imag = residual[row - column]
            lower[row][column] = (real / pivot, imag / pivot)
    inverse = [[None] * order for _ in range(order)]
    for row in range(order):
        pivot = lower[row][row][0]
        inverse[row][row] = (1.0 / pivot, jnp.zeros_like(pivot))
        for column in range(row):
            real = jnp.zeros_like(pivot)
            imag = jnp.zeros_like(pivot)
            for k in range(column, row):
                a, b = lower[row][k]
                c, d = inverse[k][column]
                real = real - (a * c - b * d)
                imag = imag - (a * d + b * c)
            inverse[row][column] = (real / pivot, imag / pivot)
    return inverse


def split_table(table):
    high = table.astype(jnp.bfloat16)
    low = (table - high.astype(np.float64)).astype(jnp.bfloat16)
    return high, low


def right_table(extent, sign):
    grid = np.outer(np.arange(extent), np.arange(extent)) % extent
    angle = 2.0 * math.pi / extent * grid
    cosine, sine = np.cos(angle), sign * np.sin(angle)
    table = np.block([[cosine, sine], [-sine, cosine]])
    high, low = split_table(table)
    upper = np.concatenate([high, low], axis=1)
    lower = np.concatenate([high, np.zeros_like(low)], axis=1)
    return np.concatenate([upper, lower], axis=0)


def left_table(extent, sign):
    grid = np.outer(np.arange(extent), np.arange(extent)) % extent
    angle = 2.0 * math.pi / extent * grid
    high, low = split_table(np.concatenate([np.cos(angle), sign * np.sin(angle)], axis=0))
    return np.concatenate([high, high, low], axis=1)


def halves(value):
    high = value.astype(jnp.bfloat16)
    low = (value - high.astype(jnp.float32)).astype(jnp.bfloat16)
    return high, low


def right_product(value, table):
    lanes = value.shape[-1]
    high, low = halves(value)
    both = jnp.dot(
        jnp.concatenate([high, low], axis=1), table, preferred_element_type=jnp.float32
    )
    return both[:, :lanes] + both[:, lanes:]


def left_product(first, second, table):
    rows, lanes = first.shape
    high, low = halves(jnp.concatenate([first, second], axis=1))
    stacked = jnp.concatenate([high, low, high], axis=0)
    both = jnp.dot(table, stacked, preferred_element_type=jnp.float32)
    return tuple(
        both[:rows, cut : cut + lanes] - turn(both[rows:, cut : cut + lanes])
        for cut in (0, lanes)
    )


def spread_parts(value):
    lanes = value.shape[-1]
    swapped = pltpu.roll(value, lanes // 2, value.ndim - 1)
    lower = lax.broadcasted_iota(jnp.int32, value.shape, value.ndim - 1) < lanes // 2
    return jnp.where(lower, value, swapped), jnp.where(lower, swapped, value)


def forward_group(group, orbital_grid, partner_grid, work, right, left):
    rows, lanes = orbital_grid.shape[1:]
    span = pl.ds(group * GROUP, GROUP)
    orbital = orbital_grid[span].reshape(GROUP * rows, lanes)
    real, imag = spread_parts(partner_grid[span].reshape(GROUP * rows, lanes))
    density = real * orbital + imag * turn(orbital)
    lines = right_product(density, right[...])
    planes = []
    for pair in range(GROUP // 2):
        start = 2 * pair * rows
        planes += left_product(
            lines[start : start + rows], lines[start + rows : start + 2 * rows], left[...]
        )
    stacked = jnp.stack(planes, axis=0)
    work[:, span, :] = jnp.swapaxes(stacked, 0, 1)


def backward_group(group, partner_grid, partial, work, right, left):
    rows, lanes = partner_grid.shape[1:]
    span = pl.ds(group * GROUP, GROUP)
    planes = jnp.swapaxes(work[:, span, :], 0, 1)
    lines = []
    for pair in range(GROUP // 2):
        lines += left_product(planes[2 * pair], planes[2 * pair + 1], left[...])
    field = right_product(jnp.concatenate(lines, axis=0), right[...])
    real, imag = spread_parts(partner_grid[span].reshape(GROUP * rows, lanes))
    partial[span] = (real * field - imag * turn(field)).reshape(GROUP, rows, lanes)


def middle_pairs(shift, work, forward, inverse):
    columns, extent, lanes = work.shape
    first = frequency(lax.broadcasted_iota(jnp.int32, (extent, lanes), 0), extent)
    third_place = lax.broadcasted_iota(jnp.int32, (extent, lanes), 1)
    third_place = jnp.where(third_place < lanes // 2, third_place, third_place - lanes // 2)
    third = frequency(third_place, extent)
    base = (first + shift[0]) ** 2 + (third + shift[2]) ** 2 + SCREEN_SQUARE
    scale = FOUR_PI / (float(extent) * float(columns) * float(lanes // 2))

    def one_pair(pair, carry):
        spectra = left_product(work[2 * pair], work[2 * pair + 1], forward[...])
        scaled = []
        for which in range(2):
            column = 2 * pair + which
            second = jnp.where(column < columns // 2, column, column - columns)
            offset = (second.astype(jnp.float32) + shift[1]) ** 2
            scaled.append(spectra[which] * (scale / (base + offset)))
        fields = left_product(scaled[0], scaled[1], inverse[...])
        work[2 * pair] = fields[0]
        work[2 * pair + 1] = fields[1]
        return carry

    lax.fori_loop(0, columns // 2, one_pair, 0, unroll=4)


def exchange_kernel(
    bands,
    ranks,
    shift_table,
    shift_index,
    orbital_home,
    partner_home,
    right_forward_home,
    right_inverse_home,
    left_forward_home,
    left_inverse_home,
    potential,
    projector,
    orbital_grid,
    partner_grid,
    orbital_parts,
    from_below,
    from_above,
    work,
    partial,
    near,
    outgoing,
    arriving,
    potential_parts,
    projector_parts,
    own_sums,
    all_sums,
    chain_send,
    chain_recv,
    deliver_send,
    deliver_recv,
    grid_send,
    grid_recv,
    early_send,
    early_recv,
    local_sem,
    near_send,
    near_recv,
    far_send,
    far_recv,
    part_send,
    part_recv,
    sum_send,
    sum_recv,
    back_send,
    back_recv,
    orbital,
    partner,
    right_forward,
    right_inverse,
    left_forward,
    left_inverse,
    load_sem,
):
    loads = [
        pltpu.make_async_copy(home, here, load_sem.at[number])
        for number, (home, here) in enumerate(
            (
                (partner_home, partner),
                (orbital_home, orbital),
                (right_forward_home, right_forward),
                (left_forward_home, left_forward),
                (right_inverse_home, right_inverse),
                (left_inverse_home, left_inverse),
            )
        )
    ]
    for load in loads:
        load.start()
    band = lax.axis_index("band")
    rank = lax.axis_index("fft")
    planes, rows, lanes = orbital.shape
    piece = planes // bands
    per_group = GROUP // piece
    halves_count = planes // GROUP
    greet(
        [
            {"band": (band + step) % bands, "fft": (rank + turn_by) % ranks}
            for step in range(bands)
            for turn_by in range(ranks)
            if step or turn_by
        ]
    )
    loads[0].wait()

    def span(index):
        return pl.ds(index * piece, piece)

    def slab(index):
        return pl.ds(index * planes, planes)

    beside = rank + 1 - 2 * (rank % 2)
    across = (rank + 2) % ranks
    beside_across = (beside + 2) % ranks

    def chain_copy(upward, distance, chunk):
        held = from_below if upward else from_above
        source = partner.at[span(chunk)] if distance == 0 else held.at[distance - 1, chunk]
        way = 0 if upward else 1
        return remote(
            source,
            held.at[distance, chunk],
            chain_send.at[way, distance, chunk],
            chain_recv.at[way, distance, chunk],
            {"band": band + 1 if upward else band - 1},
        )

    def deliver(upward, distance, chunk, act):
        held = from_below if upward else from_above
        source = partner.at[span(chunk)] if distance == 0 else held.at[distance - 1, chunk]
        owner = band - distance if upward else band + distance
        target = partner_grid.at[pl.ds(rank * planes + chunk * piece, piece)]
        way = 0 if upward else 1

        @pl.when(owner == rank)
        def _():
            if act == "start":
                pltpu.make_async_copy(source, target, local_sem.at[chunk]).start()

        @pl.when(owner != rank)
        def _():
            copy = remote(
                source,
                target,
                deliver_send.at[way, distance, chunk],
                deliver_recv.at[rank, chunk],
                {"fft": owner},
            )
            copy.start() if act == "start" else copy.wait_send()

    def has_source(upward, distance):
        return band >= distance if upward else band + distance <= bands - 1

    def has_next(upward):
        return band <= bands - 2 if upward else band >= 1

    def both(first, second):
        return jnp.logical_and(first, second)

    def forward_half(half):
        for chunk in range(half * per_group, (half + 1) * per_group):
            target = partner_grid.at[pl.ds(rank * planes + chunk * piece, piece)]
            pltpu.make_async_copy(partner.at[span(chunk)], target, local_sem.at[chunk]).wait()
            for step in range(1, ranks):
                source = (rank + step) % ranks
                target = partner_grid.at[pl.ds(source * planes + chunk * piece, piece)]
                remote(
                    target,
                    target,
                    deliver_send.at[0, 0, chunk],
                    deliver_recv.at[source, chunk],
                    {"fft": source},
                ).wait_recv()

        def forward(index, carry):
            forward_group(
                index * halves_count + half,
                orbital_grid,
                partner_grid,
                work,
                right_forward,
                left_forward,
            )
            return carry

        lax.fori_loop(0, ranks, forward, 0)

    for chunk in range(bands):
        for upward in (True, False):

            @pl.when(has_next(upward))
            def _():
                chain_copy(upward, 0, chunk).start()

    loads[1].wait()
    to_across = remote(
        orbital, orbital_grid.at[slab(rank)], grid_send.at[0], grid_recv.at[0], {"fft": across}
    )
    to_beside = remote(
        orbital, orbital_grid.at[slab(rank)], grid_send.at[1], grid_recv.at[1], {"fft": beside}
    )
    to_across.start()
    to_beside.start()
    own_grid = pltpu.make_async_copy(orbital, orbital_grid.at[slab(rank)], local_sem.at[bands])
    own_grid.start()
    for chunk in range(bands):
        deliver(True, 0, chunk, "start")
    onward = remote(
        orbital_grid.at[slab(across)],
        orbital_grid.at[slab(across)],
        grid_send.at[2],
        grid_recv.at[2],
        {"fft": beside},
    )
    for distance in range(1, bands):
        for chunk in range(bands):
            for upward in (True, False):

                @pl.when(has_source(upward, distance))
                def _():
                    chain_copy(upward, distance - 1, chunk).wait_recv()

                if distance < bands - 1:

                    @pl.when(both(has_source(upward, distance), has_next(upward)))
                    def _():
                        chain_copy(upward, distance, chunk).start()

                @pl.when(has_source(upward, distance))
                def _():
                    deliver(upward, distance, chunk, "start")

            if distance == bands - 1 and chunk > 0 and chunk % per_group == 0:
                forward_half(chunk // per_group - 1)

        if distance == 1:
            to_across.wait_recv()
            onward.start()
            own_grid.wait()
            for load in loads[2:]:
                load.wait()
            to_beside.wait_recv()
            onward.wait_recv()
    forward_half(halves_count - 1)
    early_copies = []
    for step in range(1, bands):
        other = (band + step) % bands
        copy = remote(
            orbital.at[span(other)],
            orbital_parts.at[band],
            early_send.at[step - 1],
            early_recv.at[step - 1],
            {"band": other},
        )
        copy.start()
        early_copies.append(copy)
    own_part = pltpu.make_async_copy(
        orbital.at[span(band)], orbital_parts.at[band], local_sem.at[bands + 1]
    )
    own_part.start()

    chosen = shift_index[rank]
    shift = [shift_table[chosen, axis] for axis in range(3)]
    middle_pairs(shift, work, left_forward, left_inverse)

    def backward_slab(index):
        def backward(half, carry):
            backward_group(
                index * halves_count + half, partner_grid, partial, work, right_inverse, left_inverse
            )
            return carry

        lax.fori_loop(0, halves_count, backward, 0)

    def near_copy(which, index):
        return remote(
            partial.at[slab(index)],
            near.at[which],
            near_send.at[which],
            near_recv.at[which],
            {"fft": beside},
        )

    def far_copy(chunk):
        return remote(
            outgoing.at[chunk],
            arriving.at[chunk],
            far_send.at[chunk],
            far_recv.at[chunk],
            {"fft": across},
        )

    def window(index, chunk):
        return pl.ds(index * planes + chunk * piece, piece)

    turns = [(band + step) % bands for step in range(1, bands + 1)]
    backward_slab(beside_across)
    near_copy(1, beside_across).start()
    backward_slab(across)
    near_copy(1, beside_across).wait_recv()
    for chunk in turns:
        outgoing[chunk] = partial[window(across, chunk)] + near[1, span(chunk)]
        far_copy(chunk).start()
    backward_slab(beside)
    near_copy(0, beside).start()
    backward_slab(rank)
    near_copy(0, beside).wait_recv()

    def part_copy(chunk):
        return remote(
            potential.at[span(chunk)],
            potential_parts.at[band],
            part_send.at[chunk],
            part_recv.at[band],
            {"band": chunk},
        )

    for step, chunk in enumerate(turns):
        far_copy(chunk).wait_recv()
        potential[span(chunk)] = (
            partial[window(rank, chunk)] + near[0, span(chunk)]
        ) + arriving[chunk]
        if step < bands - 1:
            part_copy(chunk).start()
        else:
            potential_parts[band] = potential[span(band)]
    for chunk in turns[:-1]:
        remote(
            potential_parts.at[chunk],
            potential_parts.at[chunk],
            part_send.at[chunk],
            part_recv.at[chunk],
            {"band": chunk},
        ).wait_recv()
    for copy in early_copies:
        copy.wait()
    own_part.wait()

    entries = [(i, l) for i in range(bands) for l in range(i + 1)]
    position = lax.broadcasted_iota(jnp.int32, (8, lanes), 1)

    def accumulate(plane, sums):
        turned = []
        straight = []
        for l in range(bands):
            block = potential_parts[l, plane]
            straight.append(block)
            turned.append(turn(block))
        result = []
        for number, (i, l) in enumerate(entries):
            left = orbital_parts[i, plane]
            for half, right in enumerate((straight[l], turned[l])):
                product = (left * right).reshape(rows // 8, 8, lanes)
                result.append(sums[2 * number + half] + jnp.sum(product, axis=0))
        return tuple(result)

    zero = jnp.zeros((8, lanes), jnp.float32)
    sums = lax.fori_loop(0, piece, accumulate, (zero,) * (2 * len(entries)))
    packed = zero
    for number, value in enumerate(sums):
        packed = jnp.where(position == number, jnp.sum(value, axis=1, keepdims=True), packed)
    own_sums[...] = packed
    sum_copies = []
    number = 0
    for step in range(bands):
        for turn_by in range(ranks):
            if step == 0 and turn_by == 0:
                continue
            copy = remote(
                own_sums,
                all_sums.at[band, rank],
                sum_send.at[step, turn_by],
                sum_recv.at[step, turn_by],
                {"band": (band + step) % bands, "fft": (rank + turn_by) % ranks},
            )
            copy.start()
            sum_copies.append(copy)
    all_sums[band, rank] = packed
    for copy in sum_copies:
        copy.wait()
    total = zero
    for one_band in range(bands):
        for one_rank in range(ranks):
            total = total + all_sums[one_band, one_rank]
    total = jnp.broadcast_to(jnp.sum(total, axis=0, keepdims=True), (8, lanes))
    volume = float(lanes // 2) * float(rows) * float(planes * ranks)
    matrix = [[None] * bands for _ in range(bands)]
    for number, (i, l) in enumerate(entries):
        values = [
            jnp.broadcast_to(
                jnp.sum(jnp.where(position == 2 * number + half, total, 0.0), axis=1, keepdims=True),
                (8, lanes),
            )
            / volume
            for half in range(2)
        ]
        matrix[i][l] = (values[0], values[1])
    inverse = small_factor_inverse(matrix)
    back_copies = []

    def spread(value):
        return value[:1]

    for l in range(bands):

        def combine(plane, carry):
            sum_straight = jnp.zeros((rows, lanes), jnp.float32)
            sum_turned = jnp.zeros((rows, lanes), jnp.float32)
            for m in range(l + 1):
                block = potential_parts[m, plane]
                real, imag = inverse[l][m]
                sum_straight = sum_straight + spread(real) * block
                sum_turned = sum_turned + spread(imag) * block
            projector_parts[l, plane] = sum_straight + turn(sum_turned)
            return carry

        lax.fori_loop(0, piece, combine, 0)

    for chunk in turns[1:-1] + turns[:1]:
        remote(
            projector_parts.at[chunk],
            projector.at[span(band)],
            back_send.at[chunk],
            back_recv.at[band],
            {"band": chunk},
        ).start()
    projector[span(band)] = projector_parts[band]
    for chunk in turns[:-1]:
        back = remote(
            projector_parts.at[chunk],
            projector.at[span(chunk)],
            back_send.at[chunk],
            back_recv.at[chunk],
            {"band": chunk},
        )
        back.wait_recv()
        back.wait_send()
        part_copy(chunk).wait_send()
    for chunk in turns:
        far_copy(chunk).wait_send()
    near_copy(0, beside).wait_send()
    near_copy(1, beside_across).wait_send()
    to_across.wait_send()
    to_beside.wait_send()
    onward.wait_send()
    for distance in range(bands):
        for chunk in range(bands):
            for upward in (True, False):
                if distance < bands - 1:

                    @pl.when(both(has_source(upward, distance), has_next(upward)))
                    def _():
                        chain_copy(upward, distance, chunk).wait_send()

                if distance > 0 or upward:

                    @pl.when(has_source(upward, distance))
                    def _():
                        deliver(upward, distance, chunk, "wait")


def exchange(bands, ranks, orbital, partner, shift_table, shift_index):
    planes, rows, lanes = orbital.shape
    piece = planes // bands
    vmem = pl.BlockSpec(memory_space=pltpu.VMEM)
    smem = pl.BlockSpec(memory_space=pltpu.SMEM)
    out = jax.ShapeDtypeStruct((planes, rows, lanes), jnp.float32)
    grid = pltpu.VMEM((ranks * planes, rows, lanes), jnp.float32)
    held = pltpu.VMEM((bands - 1, bands, piece, rows, lanes), jnp.float32)
    quarters = pltpu.VMEM((bands, piece, rows, lanes), jnp.float32)
    dma = pltpu.SemaphoreType.DMA
    tables = [
        jnp.asarray(table)
        for table in (
            right_table(rows, -1.0),
            right_table(rows, 1.0),
            left_table(rows, -1.0),
            left_table(rows, 1.0),
        )
    ]
    return pl.pallas_call(
        functools.partial(exchange_kernel, bands, ranks),
        name="exchange",
        out_shape=(out, out),
        in_specs=[smem, smem] + [pl.BlockSpec(memory_space=pl.ANY)] * 6,
        out_specs=(vmem, vmem),
        scratch_shapes=[
            grid,
            grid,
            quarters,
            held,
            held,
            grid,
            grid,
            pltpu.VMEM((2, planes, rows, lanes), jnp.float32),
            quarters,
            quarters,
            quarters,
            quarters,
            pltpu.VMEM((8, lanes), jnp.float32),
            pltpu.VMEM((bands, ranks, 8, lanes), jnp.float32),
            dma((2, bands, bands)),
            dma((2, bands, bands)),
            dma((2, bands, bands)),
            dma((ranks, bands)),
            dma((3,)),
            dma((3,)),
            dma((bands,)),
            dma((bands,)),
            dma((bands + 2,)),
            dma((2,)),
            dma((2,)),
            dma((bands,)),
            dma((bands,)),
            dma((bands,)),
            dma((bands,)),
            dma((bands, ranks)),
            dma((bands, ranks)),
            dma((bands,)),
            dma((bands,)),
            pltpu.VMEM(orbital.shape, jnp.float32),
            pltpu.VMEM(orbital.shape, jnp.float32),
        ]
        + [pltpu.VMEM(table.shape, table.dtype) for table in tables]
        + [dma((6,))],
        compiler_params=pltpu.CompilerParams(
            collective_id=0, has_side_effects=True, vmem_limit_bytes=60 * 1024 * 1024
        ),
    )(shift_table, shift_index, orbital, partner, *tables)


def paired_body(bands, ranks, orbitals, partners, shift_table, shift_index):
    potential, projector = exchange(
        bands, ranks, orbitals[0], partners[0], shift_table, shift_index
    )
    return (potential[None], projector[None])


def body(orbitals, partners, shift_table, shift_index):
    bands = lax.axis_size("band")
    ranks = lax.axis_size("fft")
    count, planes, rows, lanes = orbitals.shape
    grid_bytes = ranks * planes * rows * lanes * 4
    paired = (
        count == 1
        and ranks == 4
        and bands == ranks
        and planes % bands == 0
        and planes % GROUP == 0
        and GROUP % (planes // bands) == 0
        and lanes == 2 * rows
        and lanes == 128
        and grid_bytes <= 2 * 1024 * 1024
    )
    if paired:
        return paired_body(bands, ranks, orbitals, partners, shift_table, shift_index)
    return general_body(orbitals, partners, shift_table, shift_index)


def solution(mesh):
    in_specs = (
        P(("kgrp", "band"), "fft", None, None),
        P(("kgrp", "band"), "fft", None, None),
        P(),
        P("kgrp"),
    )
    out_specs = (P(("kgrp", "band"), "fft", None, None), P(("kgrp", "band"), "fft", None, None))
    return jax.shard_map(body, mesh=mesh, in_specs=in_specs, out_specs=out_specs, check_vma=False)
```
